128 devices in a mesh: row: 8 (over y, z_lo), col: 16 (over x, z_hi, core).
Axes of the slice: x: 4, y: 4, z: 4 (z_hi: 2, z_lo: 2; z = z_hi * 2 + z_lo), core: 2. Of those that a mesh axis runs over, the one named last changes fastest.
Arguments:
- hidden_states: bfloat16 [16384, 8192], P(('row', 'col')), may hold values from -6 to 6
- w_c: bfloat16 [8192, 512], replicated, may hold values from -0.0625 to 0.0625
- w_b: bfloat16 [8192, 128], replicated, may hold values from -0.0625 to 0.0625
- teacher_q: bfloat16 [16384, 512], P(('row', 'col')), may hold values from -4 to 4
- teacher_k: bfloat16 [16384, 128], P(('row', 'col')), may hold values from -4 to 4
Outputs:
- grad_c: bfloat16 [16384, 512], P(('row', 'col'))
- grad_b: bfloat16 [16384, 128], P(('row', 'col'))
The draws below stay inside these ranges and needn't reach their ends.
All inputs are finite; a program needn't handle non-finite values.
Results may differ from the reference program's by a relative error of at most 0.0056.
Values may be sent and summed in bfloat16 or wider, within the bound.
No kernel may reach another device: no remote copies, remote signals or barrier semaphores. Data moves between devices by JAX's collectives and lax.ppermute only.
A program may use at most 128 MiB of HBM per device.

```python
import math
import jax
import jax.numpy as jnp
from jax import lax

D = 8192
HEADS = 4
HEAD = 128
TOKENS = 16384


def teacher_pair(key):
    query_seed = jax.random.fold_in(key, 101)
    key_seed = jax.random.fold_in(key, 202)
    key_rows = jnp.clip(jax.random.normal(key_seed, (TOKENS, HEAD), jnp.float32), -4.0, 4.0)
    query_rows = jnp.clip(jax.random.normal(query_seed, (TOKENS, HEADS * HEAD), jnp.float32), -4.0, 4.0)
    return (query_rows, key_rows)


def draw_teacher_q(key, part):
    return teacher_pair(key)[0].astype(jnp.bfloat16)


def draw_teacher_k(key, part):
    return teacher_pair(key)[1].astype(jnp.bfloat16)


def steps_of(rng, extent, shards, least, largest):
    factor_of, own = 1.0, jax.random.fold_in(rng, 6)
    for dim, shards_of in shards:
        draws = jnp.exp(jax.random.uniform(jax.random.fold_in(own, dim), (shards_of,), jnp.float32, least / len(shards), largest / len(shards)))
        factor_of = factor_of * jnp.repeat(draws, extent[dim] // shards_of).reshape([-1 if axis == dim else 1 for axis in range(len(extent))])
    return factor_of


def bell_draw(own_key, shape, width, bound, cuts=(), kind=jnp.bfloat16):
    drawn = jax.random.normal(own_key, shape, jnp.float32) * width
    if len(cuts) > 0:
        drawn = steps_of(own_key, shape, cuts, -0.22, 0.18) * drawn
    return jnp.clip(drawn, min=-bound, max=bound).astype(kind)


def setup_inputs(seed: int = 0) -> dict:
    key_list = jax.random.split(jax.random.key(seed), 6)
    hidden_states = bell_draw(key_list[0], (TOKENS, D), 1.0, 6.0, ((0, 128),))
    w_c = bell_draw(key_list[1], (D, HEADS * HEAD), D ** -0.5, 0.0625)
    w_b = bell_draw(key_list[2], (D, HEAD), D ** -0.5, 0.0625)
    teacher_q = draw_teacher_q(jax.random.fold_in(key_list[5], 71), 0)
    teacher_k = draw_teacher_k(jax.random.fold_in(key_list[5], 71), 0)
    return dict(hidden_states=hidden_states, w_c=w_c, w_b=w_b, teacher_q=teacher_q, teacher_k=teacher_k)


LOSS_GAIN = 16.0
LENGTH_BASE = 512.0
NEGATIVE = -1e+30

def reference(hidden_states, w_c, w_b, teacher_q, teacher_k):
    c_proj = jnp.dot(hidden_states, w_c, preferred_element_type=jnp.float32).astype(jnp.bfloat16)
    b_proj = jnp.dot(hidden_states, w_b, preferred_element_type=jnp.float32).astype(jnp.bfloat16)
    height = math.gcd(512, TOKENS)
    row_parts = []
    grad_keys = jnp.zeros((TOKENS, HEAD), jnp.float32)
    for offset in range(0, TOKENS, height):
        finish = offset + height
        queries = teacher_q[offset:finish].astype(jnp.float32).reshape(height, HEADS, HEAD)
        c_rows = c_proj[offset:finish].astype(jnp.float32).reshape(height, HEADS, HEAD)
        key_rows = teacher_k[:finish].astype(jnp.float32)
        b_rows = b_proj[:finish].astype(jnp.float32)
        query_pos = jnp.arange(offset, finish, dtype=jnp.int32)
        key_pos = jnp.arange(finish, dtype=jnp.int32)
        visible = key_pos[None, None, :] <= query_pos[None, :, None]
        temper = jnp.log(query_pos.astype(jnp.float32) + 2.0) / (math.log(LENGTH_BASE) * math.sqrt(HEAD))
        logits = jnp.einsum('qhp,kp->hqk', queries, key_rows) * temper[None, :, None]
        logits = jnp.where(visible, logits, NEGATIVE)
        peak = lax.optimization_barrier(jnp.max(logits, axis=2))
        weights = jnp.where(visible, jnp.exp(logits - peak[:, :, None]), 0.0)
        total = lax.optimization_barrier(jnp.sum(weights, axis=2))
        probs = weights / total[:, :, None]
        student = jnp.einsum('qhp,kp->hqk', c_rows, b_rows)
        student = student / (math.sqrt(HEAD) * (query_pos.astype(jnp.float32) + 1.0))[None, :, None]
        error = jnp.where(visible, student - probs, 0.0).astype(jnp.bfloat16)
        error = lax.optimization_barrier(error).astype(jnp.float32)
        row_parts.append(jnp.einsum('hqk,kp->qhp', error, b_rows).reshape(height, HEADS * HEAD))
        grad_keys = grad_keys.at[:finish].add(jnp.einsum('hqk,qhp->kp', error, c_rows))
    factor = LOSS_GAIN / math.sqrt(HEAD)
    grad_c = (jnp.concatenate(row_parts, axis=0) * factor).astype(jnp.bfloat16)
    grad_b = (grad_keys * factor).astype(jnp.bfloat16)
    return (grad_c, grad_b)
```

```python
import functools
import math

import jax
import jax.numpy as jnp
from jax import lax
from jax.experimental import pallas as pl
from jax.experimental.pallas import tpu as pltpu
from jax.sharding import Mesh, PartitionSpec as P

HEADS = 4
HEAD = 128
TOK = 128
LOSS_GAIN = 16.0
LENGTH_BASE = 512.0
LOG2E = math.log2(math.e)

AXES = ("y", "zl", "x", "zh", "c")
SIZES = (4, 2, 4, 2, 2)
PLANE = ("zl", "x", "zh")
PLANE_N = 16
RING = 4
HALF = PLANE_N * TOK
BLOCK = 2 * HALF
ROWS = HEADS * TOK
TILE = 512
TILES = HALF // TILE
MASKED = -1e30
LOWEST = -1e29


NT = (((1,), (1,)), ((), ()))
NN = (((1,), (0,)), ((), ()))
TN = (((0,), (0,)), ((), ()))


def mxu(a, b, dims):
    return lax.dot_general(a, b, dims, preferred_element_type=jnp.float32)


def stack_heads(dst, slot, src):
    for h in range(HEADS):
        dst[slot, h * TOK:(h + 1) * TOK, :] = src[:, h * HEAD:(h + 1) * HEAD]


def query_rows(first):
    lane = lax.broadcasted_iota(jnp.int32, (1, ROWS), 1)
    return first + (lane & (TOK - 1))


def temper(pos):
    scale = LOG2E / (math.log(LENGTH_BASE) * math.sqrt(HEAD))
    return jnp.log(pos.astype(jnp.float32) + 2.0) * scale


def visible(tile, core, query):
    row = lax.broadcasted_iota(jnp.int32, (TILE, 1), 0)
    group = tile * (TILE // TOK) + (row >> 7)
    key = (group * 2 + core) * TOK + (row & (TOK - 1))
    return key <= query


def stats_kernel(s_ref, km_ref, ko_ref, q0, q1, q2, q3, out_ref, qs):
    y, group, core = s_ref[0], s_ref[1], s_ref[2]
    offset = (group * 2 + core) * TOK
    for k, q in enumerate((q0, q1, q2, q3)):
        stack_heads(qs, k, q)
    for k in range(RING):
        out_ref[k, 0:1, :] = jnp.full((1, ROWS), LOWEST, jnp.float32)
        out_ref[k, 1:2, :] = jnp.zeros((1, ROWS), jnp.float32)

    def step(scale, query, keys, tile, which, state):
        peak, total = state
        logits = mxu(keys, query, NT) * scale
        if which is not None:
            logits = jnp.where(which, logits, MASKED)
        cut = logits.reshape(TILE // 8, 8, ROWS)
        newest = jnp.maximum(peak, jnp.max(cut, axis=0))
        part = jnp.sum(jnp.exp2(cut - newest[None]), axis=0)
        return newest, total * jnp.exp2(peak - newest) + part

    def finish(chunk, state):
        peak, total = state
        best = jnp.max(peak, axis=0, keepdims=True)
        out_ref[chunk, 0:1, :] = best
        out_ref[chunk, 1:2, :] = jnp.sum(total * jnp.exp2(peak - best), axis=0, keepdims=True)

    start = (jnp.full((8, ROWS), LOWEST, jnp.float32), jnp.zeros((8, ROWS), jnp.float32))

    def own(tile, state):
        scale = temper(query_rows(y * BLOCK + offset))
        local = query_rows(offset)
        row = pl.multiple_of(tile * TILE, TILE)
        query = qs[0]
        state = step(scale, query, km_ref[pl.ds(row, TILE), :], tile, visible(tile, core, local), state)
        return step(scale, query, ko_ref[pl.ds(row, TILE), :], tile, visible(tile, 1 - core, local), state)

    finish(y, lax.fori_loop(0, group // (TILE // TOK) + 1, own, start))

    def later(k, unused):
        scale = temper(query_rows((y + k) * BLOCK + offset))

        def inner(tile, state):
            row = pl.multiple_of(tile * TILE, TILE)
            query = qs[k]
            state = step(scale, query, km_ref[pl.ds(row, TILE), :], tile, None, state)
            return step(scale, query, ko_ref[pl.ds(row, TILE), :], tile, None, state)

        finish(y + k, lax.fori_loop(0, TILES, inner, start))
        return unused

    lax.fori_loop(1, RING - y, later, 0)


def error_kernel(s_ref, km_ref, ko_ref, bm_ref, bo_ref, q0, q1, q2, q3, c0, c1, c2, c3,
                 t0, t1, t2, t3, o0, o1, o2, o3, gm_ref, go_ref, qs, cs, acc, sums, lse):
    y, group, core = s_ref[0], s_ref[1], s_ref[2]
    offset = (group * 2 + core) * TOK
    factor = LOSS_GAIN / math.sqrt(HEAD)
    for k, (q, c) in enumerate(((q0, c0), (q1, c1), (q2, c2), (q3, c3))):
        stack_heads(qs, k, q)
        stack_heads(cs, k, c)
        acc[k] = jnp.zeros((HEAD, ROWS), jnp.float32)
        best = functools.reduce(jnp.maximum, [t[k, 0:1, :] for t in (t0, t1, t2, t3)])
        total = sum(t[k, 1:2, :] * jnp.exp2(t[k, 0:1, :] - best) for t in (t0, t1, t2, t3))
        lse[k] = best + jnp.log(total) * LOG2E
    sums[...] = jnp.zeros((2, HALF, HEAD), jnp.float32)

    def step(k, tile, half, keys_ref, bs_ref, which):
        pos = query_rows((y + k) * BLOCK + offset)
        row = pl.multiple_of(tile * TILE, TILE)
        keys, bs = keys_ref[pl.ds(row, TILE), :], bs_ref[pl.ds(row, TILE), :]
        crow = cs[k]
        probs = jnp.exp2(mxu(keys, qs[k], NT) * temper(pos) - lse[y + k])
        student = mxu(bs, crow, NT) * (1.0 / (math.sqrt(HEAD) * (pos.astype(jnp.float32) + 1.0)))
        error = student - probs
        if which is not None:
            error = jnp.where(which, error, 0.0)
        error = error.astype(jnp.bfloat16)
        acc[k] += mxu(bs, error, TN)
        sums[half, pl.ds(row, TILE), :] += mxu(error, crow, NN)

    def own(tile, unused):
        local = query_rows(offset)
        step(0, tile, 0, km_ref, bm_ref, visible(tile, core, local))
        step(0, tile, 1, ko_ref, bo_ref, visible(tile, 1 - core, local))
        return unused

    lax.fori_loop(0, group // (TILE // TOK) + 1, own, 0)

    def later(k, unused):
        def inner(tile, unused):
            step(k, tile, 0, km_ref, bm_ref, None)
            step(k, tile, 1, ko_ref, bo_ref, None)
            return unused

        return lax.fori_loop(0, TILES, inner, unused)

    lax.fori_loop(1, RING - y, later, 0)

    for k, o in enumerate((o0, o1, o2, o3)):
        for h in range(HEADS):
            piece = acc[k, :, h * TOK:(h + 1) * TOK].T * factor
            o[:, h * HEAD:(h + 1) * HEAD] = piece.astype(o.dtype)
    gm_ref[...] = sums[0] * factor
    go_ref[...] = (sums[1] * factor).astype(jnp.bfloat16)


def down(value, k):
    return lax.ppermute(value, "y", [(s, s - k) for s in range(k, RING)])


def up(value, k):
    return lax.ppermute(value, "y", [(s, s + k) for s in range(RING - k)])


def around(value, k):
    return lax.ppermute(value, "y", [(s, (s + k) % RING) for s in range(RING)])


def swap(value):
    return lax.ppermute(value, "c", [(0, 1), (1, 0)])


def exchange(value):
    return lax.all_to_all(value, PLANE, 0, 0, tiled=True)


def on_device(hidden_states, w_c, w_b, teacher_q, teacher_k):
    y, core = lax.axis_index("y"), lax.axis_index("c")
    group = (lax.axis_index("zl") * 4 + lax.axis_index("x")) * 2 + lax.axis_index("zh")
    place = jnp.stack([y, group, core]).astype(jnp.int32)

    k_mine = exchange(jnp.tile(teacher_k, (PLANE_N, 1)))
    queries = [teacher_q] + [down(teacher_q, k) for k in (1, 2, 3)]
    b_proj = jnp.dot(hidden_states, w_b, preferred_element_type=jnp.float32).astype(jnp.bfloat16)
    b_mine = exchange(jnp.tile(b_proj, (PLANE_N, 1)))
    c_proj = jnp.dot(hidden_states, w_c, preferred_element_type=jnp.float32).astype(jnp.bfloat16)
    crows = [c_proj] + [down(c_proj, k) for k in (1, 2, 3)]
    k_other = swap(k_mine)
    b_other = swap(b_mine)

    vmem = pl.BlockSpec(memory_space=pltpu.VMEM)
    smem = pl.BlockSpec(memory_space=pltpu.SMEM)
    stats = pl.pallas_call(
        stats_kernel,
        out_shape=jax.ShapeDtypeStruct((RING, 2, ROWS), jnp.float32),
        in_specs=[smem] + [vmem] * 6,
        out_specs=vmem,
        scratch_shapes=[pltpu.VMEM((RING, ROWS, HEAD), jnp.bfloat16)],
        name="stats",
    )(place, k_mine, k_other, *queries)
    all_stats = [stats] + [around(stats, k) for k in (1, 2, 3)]

    part = jax.ShapeDtypeStruct((TOK, ROWS), jnp.bfloat16)
    o0, o1, o2, o3, g_mine, g_other = pl.pallas_call(
        error_kernel,
        out_shape=(
            jax.ShapeDtypeStruct((TOK, ROWS), jnp.float32), part, part, part,
            jax.ShapeDtypeStruct((HALF, HEAD), jnp.float32),
            jax.ShapeDtypeStruct((HALF, HEAD), jnp.bfloat16),
        ),
        in_specs=[smem] + [vmem] * 16,
        out_specs=(vmem,) * 6,
        scratch_shapes=[
            pltpu.VMEM((RING, ROWS, HEAD), jnp.bfloat16),
            pltpu.VMEM((RING, ROWS, HEAD), jnp.bfloat16),
            pltpu.VMEM((RING, HEAD, ROWS), jnp.float32),
            pltpu.VMEM((2, HALF, HEAD), jnp.float32),
            pltpu.VMEM((RING, 1, ROWS), jnp.float32),
        ],
        name="errors",
    )(place, k_mine, k_other, b_mine, b_other, *queries, *crows, *all_stats)

    g_sum = (g_mine + swap(g_other).astype(jnp.float32)).astype(jnp.bfloat16)
    g_parts = exchange(g_sum).reshape(PLANE_N, TOK, HEAD)
    rows = o0
    for k, o in ((1, o1), (2, o2), (3, o3)):
        rows = rows + up(o, k).astype(jnp.float32)
    grad_b = jnp.sum(g_parts.astype(jnp.float32), axis=0)
    return rows.astype(jnp.bfloat16), grad_b.astype(jnp.bfloat16)


def solution(mesh):
    inner = Mesh(mesh.devices.reshape(SIZES), AXES)
    tokens = P(AXES, None)
    return jax.shard_map(
        on_device,
        mesh=inner,
        in_specs=(tokens, P(), P(), tokens, tokens),
        out_specs=(tokens, tokens),
        check_vma=False,
    )
```

```python
import functools
import math

import jax
import jax.numpy as jnp
from jax import lax
from jax.experimental import pallas as pl
from jax.experimental.pallas import tpu as pltpu
from jax.sharding import Mesh, PartitionSpec as P


HEADS = 4
HEAD = 128
TOK = 128
LOSS_GAIN = 16.0
LENGTH_BASE = 512.0
LOG2E = math.log2(math.e)

AXES = ("y", "zl", "x", "zh", "c")
SIZES = (4, 2, 4, 2, 2)
PLANE = ("zl", "x", "zh")
PLANE_N = 16
RING = 4
HALF = PLANE_N * TOK
BLOCK = 2 * HALF
ROWS = HEADS * TOK
TILE = 512
TILES = HALF // TILE
MASKED = -1e30
LOWEST = -1e29
TOO_LARGE = 2.0 ** 60
VMEM_LIMIT = 20 * 1024 * 1024


NT = (((1,), (1,)), ((), ()))
NN = (((1,), (0,)), ((), ()))
TN = (((0,), (0,)), ((), ()))


def mxu(a, b, dims):
    return lax.dot_general(a, b, dims, preferred_element_type=jnp.float32)


def stack_heads(dst, slot, src):
    for h in range(HEADS):
        dst[slot, h * TOK:(h + 1) * TOK, :] = src[:, h * HEAD:(h + 1) * HEAD]


def query_rows(first):
    lane = lax.broadcasted_iota(jnp.int32, (1, ROWS), 1)
    return first + (lane & (TOK - 1))


def temper(pos):
    scale = LOG2E / (math.log(LENGTH_BASE) * math.sqrt(HEAD))
    return jnp.log(pos.astype(jnp.float32) + 2.0) * scale


def visible(tile, core, query):
    row = lax.broadcasted_iota(jnp.int32, (TILE, 1), 0)
    group = tile * (TILE // TOK) + (row >> 7)
    key = (group * 2 + core) * TOK + (row & (TOK - 1))
    return key <= query


def rows_of(ref, tile, first):
    pieces = TILE // TOK
    return ref[pl.ds(tile * pieces, pieces), first:first + TOK].reshape(TILE, HEAD)


def place():
    group = (lax.axis_index("zl") * 4 + lax.axis_index("x")) * 2 + lax.axis_index("zh")
    core = lax.axis_index("c")
    return lax.axis_index("y"), group, core, (group * 2 + core) * TOK


def weights_kernel(km_ref, ko_ref, q0, q1, q2, q3, p_ref, peak_ref, out_ref, qs, sums):
    y, group, core, offset = place()
    for k, q in enumerate((q0, q1, q2, q3)):
        stack_heads(qs, k, q)
    for k in range(RING):
        out_ref[k, 0:1, :] = jnp.full((1, ROWS), LOWEST, jnp.float32)
        out_ref[k, 1:2, :] = jnp.zeros((1, ROWS), jnp.float32)
    local = query_rows(offset)

    def masks_of(tile):
        return visible(tile, core, local), visible(tile, 1 - core, local)

    def quick(k, tiles, own):
        scale = temper(query_rows((y + k) * BLOCK + offset))
        some = mxu(km_ref[0, :TOK], qs[k], NT) * scale
        if own:
            key = core * TOK + lax.broadcasted_iota(jnp.int32, (TOK, 1), 0)
            some = jnp.where(key <= local, some, MASKED)
        level = jnp.max(some, axis=0, keepdims=True)

        def inner(tile, total):
            row = pl.multiple_of(tile * TILE, TILE)
            for half, keys_ref in enumerate((km_ref, ko_ref)):
                weight = jnp.exp2(mxu(rows_of(keys_ref, tile, 0), qs[k], NT) * scale - level)
                if own:
                    weight = jnp.where(masks_of(tile)[half], weight, 0.0)
                p_ref[k, pl.ds(half * HALF + row, TILE), :] = weight.astype(jnp.bfloat16)
                total = total + jnp.sum(weight.reshape(TILE // 8, 8, ROWS), axis=0)
            return total

        total = lax.fori_loop(0, tiles, inner, jnp.zeros((8, ROWS), jnp.float32))
        total = jnp.sum(total, axis=0, keepdims=True)
        peak_ref[k] = jnp.broadcast_to(level, (2 * TILES, ROWS))
        out_ref[y + k, 0:1, :] = level
        out_ref[y + k, 1:2, :] = total
        return jnp.max(total) > TOO_LARGE

    def careful(k, tiles, own):
        scale = temper(query_rows((y + k) * BLOCK + offset))
        peak_ref[k] = jnp.full((2 * TILES, ROWS), LOWEST, jnp.float32)
        sums[...] = jnp.zeros((2 * TILES, ROWS), jnp.float32)

        def inner(tile, unused):
            row = pl.multiple_of(tile * TILE, TILE)
            for half, keys_ref in enumerate((km_ref, ko_ref)):
                logits = mxu(rows_of(keys_ref, tile, 0), qs[k], NT) * scale
                if own:
                    logits = jnp.where(masks_of(tile)[half], logits, MASKED)
                peak = jnp.maximum(jnp.max(logits, axis=0, keepdims=True), LOWEST)
                weight = jnp.exp2(logits - peak)
                p_ref[k, pl.ds(half * HALF + row, TILE), :] = weight.astype(jnp.bfloat16)
                peak_ref[k, pl.ds(half * TILES + tile, 1), :] = peak
                sums[pl.ds(half * TILES + tile, 1), :] = jnp.sum(weight, axis=0, keepdims=True)
            return unused

        lax.fori_loop(0, tiles, inner, 0)
        peak = peak_ref[k]
        best = jnp.max(peak, axis=0, keepdims=True)
        out_ref[y + k, 0:1, :] = best
        out_ref[y + k, 1:2, :] = jnp.sum(sums[...] * jnp.exp2(peak - best), axis=0, keepdims=True)

    own_tiles = group // (TILE // TOK) + 1
    pl.when(quick(0, own_tiles, True))(lambda: careful(0, own_tiles, True))

    def later(k, unused):
        pl.when(quick(k, TILES, False))(lambda: careful(k, TILES, False))
        return unused

    lax.fori_loop(1, RING - y, later, 0)


def narrow(value):
    return value.astype(jnp.bfloat16)


def student_kernel(bm_ref, bo_ref, c0, c1, c2, c3, ct, bt, acc, sums, state):
    y, group, core, offset = place()
    last = RING - y
    below = (group * TOK, (group + core) * TOK)
    row_of = lax.broadcasted_iota(jnp.int32, (TILE, 1), 0)
    lane_of = lax.broadcasted_iota(jnp.int32, (1, TILE), 1)
    for k, c in enumerate((c0, c1, c2, c3)):
        for h in range(HEADS):
            ct[k, :, h * TOK:(h + 1) * TOK] = c[:, h * HEAD:(h + 1) * HEAD].T

    def shrink(k):
        pos = query_rows((y + k) * BLOCK + offset).astype(jnp.float32)
        return 1.0 / (math.sqrt(HEAD) * (pos + 1.0))

    before = jnp.zeros((HEAD, HEAD), jnp.float32)
    whole = jnp.zeros((HEAD, HEAD), jnp.float32)
    for half, b_ref in enumerate((bm_ref, bo_ref)):
        for tile in range(TILES):
            bs = rows_of(b_ref, tile, TOK)
            turned = bs.T
            bt[half * TILES + tile] = turned
            part = jnp.where(row_of + tile * TILE < below[half], bs, jnp.zeros_like(bs))
            before += mxu(turned, part, NN)
            whole += mxu(turned, bs, NN)

    def apply(square, k):
        high = narrow(square)
        low = narrow(square - high.astype(jnp.float32))
        return (mxu(high, ct[k], NN) + mxu(low, ct[k], NN)) * shrink(k)

    state[...] = jnp.zeros((HEAD, HEAD), jnp.float32)

    def later(k, unused):
        acc[k] = apply(whole, k)
        state[...] += mxu(ct[k], narrow(ct[k].astype(jnp.float32) * shrink(k)), NT)
        return unused

    lax.fori_loop(1, last, later, 0)
    own = mxu(ct[0], narrow(ct[0].astype(jnp.float32) * shrink(0)), NT)
    both = narrow(jnp.concatenate([state[...], own], axis=1))
    for half in range(2):
        for tile in range(TILES):
            turned = bt[half * TILES + tile]
            part = jnp.where(lane_of + tile * TILE < below[half], turned, jnp.zeros_like(turned))
            value = mxu(both, jnp.concatenate([turned, part], axis=0), NN)
            for piece in range(TILE // TOK):
                sums[half, tile * (TILE // TOK) + piece] = value[:, piece * TOK:(piece + 1) * TOK]

    bs = bm_ref[group, TOK:]
    error = mxu(bs, ct[0], NN) * shrink(0)
    inside = lax.broadcasted_iota(jnp.int32, (TOK, 1), 0) <= query_rows(0)
    error = narrow(jnp.where(inside, error, 0.0))
    sums[0, group] += mxu(ct[0], error, NT)
    acc[0] = apply(before, 0) + mxu(bs, error, TN)


def sums_kernel(p_ref, peak_ref, t0, t1, t2, t3, ct, bt, acc_in, sums_in,
                o0, o1, o2, o3, gm_ref, go_ref, acc, sums):
    y, group, _, _ = place()
    factor = LOSS_GAIN / math.sqrt(HEAD)
    last = RING - y
    stats = (t0, t1, t2, t3)
    pieces = TILE // TOK
    sums[...] = jnp.zeros(sums.shape, jnp.float32)

    def chunk(k, unused):
        best = functools.reduce(jnp.maximum, [t[y + k, 0:1, :] for t in stats])
        total = sum(t[y + k, 1:2, :] * jnp.exp2(t[y + k, 0:1, :] - best) for t in stats)
        lse = best + jnp.log(total) * LOG2E
        acc[k] = acc_in[k]

        def inner(tile, unused):
            row = pl.multiple_of(tile * TILE, TILE)
            for half in range(2):
                weights = p_ref[k, pl.ds(half * HALF + row, TILE), :]
                fit = jnp.exp2(peak_ref[k, pl.ds(half * TILES + tile, 1), :] - lse)
                acc[k] -= mxu(bt[half * TILES + tile], weights, NN) * fit
                crow = narrow(ct[k].astype(jnp.float32) * fit)
                sums[half * TILES + tile] += mxu(crow, weights, NT)
            return unused

        tiles = jnp.where(k == 0, group // pieces + 1, TILES)
        lax.fori_loop(0, tiles, inner, 0)
        return unused

    lax.fori_loop(0, last, chunk, 0)

    for k, o in enumerate((o0, o1, o2, o3)):
        @pl.when(k < last)
        def _():
            for h in range(HEADS):
                piece = acc[k, :, h * TOK:(h + 1) * TOK].T * factor
                o[:, h * HEAD:(h + 1) * HEAD] = piece.astype(o.dtype)

        @pl.when(k >= last)
        def _():
            o[...] = jnp.zeros(o.shape, o.dtype)
    for half, g in enumerate((gm_ref, go_ref)):
        for i in range(PLANE_N):
            part = sums[half * TILES + i // pieces, :, (i % pieces) * TOK:(i % pieces + 1) * TOK]
            g[i] = ((sums_in[half, i] - part) * factor).astype(g.dtype)


def finish_kernel(g_ref, out_ref):
    out_ref[...] = narrow(jnp.sum(g_ref[...].astype(jnp.float32), axis=0).T)


def down(value, k):
    return lax.ppermute(value, "y", [(s, s - k) for s in range(k, RING)])


def up(value, k):
    return lax.ppermute(value, "y", [(s, s + k) for s in range(RING - k)])


def around(value, k):
    return lax.ppermute(value, "y", [(s, (s + k) % RING) for s in range(RING)])


def swap(value):
    return lax.ppermute(value, "c", [(0, 1), (1, 0)])


def exchange(value):
    return lax.all_to_all(value, PLANE, 0, 0, tiled=True)


def on_device(hidden_states, w_c, w_b, teacher_q, teacher_k):
    b_proj = narrow(jnp.dot(hidden_states, w_b, preferred_element_type=jnp.float32))
    mine = exchange(jnp.tile(jnp.concatenate([teacher_k, b_proj], axis=0)[None], (PLANE_N, 1, 1)))
    queries = [teacher_q] + [down(teacher_q, k) for k in (1, 2, 3)]
    c_proj = narrow(jnp.dot(hidden_states, w_c, preferred_element_type=jnp.float32))
    crows = [c_proj] + [down(c_proj, k) for k in (1, 2, 3)]
    other = swap(mine)

    def call(kernel, ins, outs, scratch):
        vmem = pl.BlockSpec(memory_space=pltpu.VMEM)
        return pl.pallas_call(
            kernel,
            out_shape=outs,
            in_specs=[vmem] * len(ins),
            out_specs=jax.tree.map(lambda unused: vmem, outs),
            scratch_shapes=[pltpu.VMEM(*s) for s in scratch],
            compiler_params=pltpu.CompilerParams(vmem_limit_bytes=VMEM_LIMIT),
        )(*ins)

    full, half = jnp.float32, jnp.bfloat16
    shaped = jax.ShapeDtypeStruct
    weights, peaks, stats = call(
        weights_kernel, (mine, other, *queries),
        (shaped((RING, BLOCK, ROWS), half), shaped((RING, 2 * TILES, ROWS), full), shaped((RING, 2, ROWS), full)),
        [((RING, ROWS, HEAD), half), ((2 * TILES, ROWS), full)],
    )
    all_stats = [stats] + [around(stats, k) for k in (1, 2, 3)]
    turned = call(
        student_kernel, (mine, other, *crows),
        (shaped((RING, HEAD, ROWS), half), shaped((2 * TILES, HEAD, TILE), half),
         shaped((RING, HEAD, ROWS), full), shaped((2, PLANE_N, HEAD, TOK), full)),
        [((HEAD, HEAD), full)],
    )
    part = shaped((TOK, ROWS), half)
    o0, o1, o2, o3, g_mine, g_other = call(
        sums_kernel, (weights, peaks, *all_stats, *turned),
        (shaped((TOK, ROWS), full), part, part, part,
         shaped((PLANE_N, HEAD, TOK), full), shaped((PLANE_N, HEAD, TOK), half)),
        [((RING, HEAD, ROWS), full), ((2 * TILES, HEAD, TILE), full)],
    )
    g_parts = exchange(narrow(g_mine + swap(g_other).astype(full)))
    rows = o0
    for k, o in ((1, o1), (2, o2), (3, o3)):
        rows = rows + up(o, k).astype(full)
    grad_b = call(finish_kernel, (g_parts,), shaped((TOK, HEAD), half), [])
    return narrow(rows), grad_b


def solution(mesh):
    inner = Mesh(mesh.devices.reshape(SIZES), AXES)
    tokens = P(AXES, None)

    return jax.shard_map(
        on_device,
        mesh=inner,
        in_specs=(tokens, P(), P(), tokens, tokens),
        out_specs=(tokens, tokens),
        check_vma=False,
    )
```

```python
import functools
import math

import jax
import jax.numpy as jnp
from jax import lax
from jax.experimental import pallas as pl
from jax.experimental.pallas import tpu as pltpu
from jax.sharding import Mesh, PartitionSpec as P


HEADS = 4
HEAD = 128
TOK = 128
LOSS_GAIN = 16.0
LENGTH_BASE = 512.0
LOG2E = math.log2(math.e)

AXES = ("y", "zl", "x", "zh", "c")
SIZES = (4, 2, 4, 2, 2)
PLANE = ("zl", "x", "zh")
PLANE_N = 16
RING = 4
HALF = PLANE_N * TOK
BLOCK = 2 * HALF
ROWS = HEADS * TOK
TILE = 512
TILES = HALF // TILE
PIECES = TILE // TOK
DEPTH = 8
MASKED = -1e30
LOWEST = -1e29
TOO_LARGE = 2.0 ** 60
VMEM_LIMIT = 20 * 1024 * 1024


NT = (((1,), (1,)), ((), ()))
NN = (((1,), (0,)), ((), ()))
TN = (((0,), (0,)), ((), ()))


def mxu(a, b, dims):
    return lax.dot_general(a, b, dims, preferred_element_type=jnp.float32)


def stack_heads(dst, slot, src):
    for h in range(HEADS):
        dst[slot, h * TOK:(h + 1) * TOK, :] = src[:, h * HEAD:(h + 1) * HEAD]


def query_rows(first):
    lane = lax.broadcasted_iota(jnp.int32, (1, ROWS), 1)
    return first + (lane & (TOK - 1))


def temper(pos):
    scale = LOG2E / (math.log(LENGTH_BASE) * math.sqrt(HEAD))
    return jnp.log(pos.astype(jnp.float32) + 2.0) * scale


def visible(tile, core, query):
    row = lax.broadcasted_iota(jnp.int32, (TILE, 1), 0)
    group = tile * PIECES + (row >> 7)
    key = (group * 2 + core) * TOK + (row & (TOK - 1))
    return key <= query


def place():
    group = (lax.axis_index("zl") * 4 + lax.axis_index("x")) * 2 + lax.axis_index("zh")
    core = lax.axis_index("c")
    return lax.axis_index("y"), group, core, (group * 2 + core) * TOK


def fetch(pairs, sems):
    copies = []
    for j, (source, target, split) in enumerate(pairs):
        size = source.shape[split] // DEPTH
        for i in range(DEPTH):
            cut = (slice(None),) * split + (pl.ds(i * size, size),)
            copies.append(pltpu.make_async_copy(source.at[cut], target.at[cut], sems.at[j * DEPTH + i]))
    for i in range(DEPTH):
        for copy in copies[i::DEPTH]:
            copy.start()
    return copies


def project(hidden, weights, copies):
    size = hidden.shape[1] // DEPTH
    total = None
    for i in range(DEPTH):
        for copy in copies[i::DEPTH]:
            copy.wait()
        part = mxu(hidden[:, i * size:(i + 1) * size], weights[i * size:(i + 1) * size, :], NN)
        total = part if total is None else total + part
    return narrow(total)


def project_b_kernel(h_ref, w_ref, k_ref, out_ref, hidden, weights, pair, sems, out_sems):
    copies = fetch(((h_ref, hidden, 1), (w_ref, weights, 0)), sems)
    pair[:TOK] = k_ref[...]
    pair[TOK:] = project(hidden, weights, copies)
    copies = [pltpu.make_async_copy(pair, out_ref.at[i], out_sems.at[i]) for i in range(PLANE_N)]
    for copy in copies:
        copy.start()
    for copy in copies:
        copy.wait()


def project_c_kernel(h_ref, w_ref, out_ref, hidden, weights, sems):
    copies = fetch(((h_ref, hidden, 1), (w_ref, weights, 0)), sems)
    out_ref[...] = project(hidden, weights, copies)


def rows_of(ref, tile, first, tiles=1):
    rows = ref[pl.ds(tile * PIECES, tiles * PIECES), first:first + TOK]
    return rows.reshape(tiles * TILE, HEAD)


def narrow(value):
    return value.astype(jnp.bfloat16)


def weights_kernel(swapped, *refs):
    keys_ref, *q_refs = refs[:1 + RING]
    given = refs[1 + RING:-5] if swapped else ()
    p_ref, level_ref, out_ref, qs, best_ref = refs[-5:]
    y, group, core, offset = place()
    for k, q in enumerate(q_refs):
        stack_heads(qs, k, q)
    for k in range(RING):
        out_ref[k, 0:1, :] = jnp.full((1, ROWS), LOWEST, jnp.float32)
        out_ref[k, 1:2, :] = jnp.zeros((1, ROWS), jnp.float32)
    local = query_rows(offset)
    side = 1 - core if swapped else core
    edge = group // PIECES

    def scale_of(k):
        return temper(query_rows((y + k) * BLOCK + offset))

    def fill(k, own, level):
        scale = scale_of(k)

        def inner(tile, total, masked=False):
            row = pl.multiple_of(tile * TILE, TILE)
            weight = jnp.exp2(mxu(rows_of(keys_ref, tile, 0), qs[k], NT) * scale - level)
            if masked:
                weight = jnp.where(visible(tile, side, local), weight, 0.0)
            p_ref[k, pl.ds(row, TILE), :] = narrow(weight)
            return total + jnp.sum(weight.reshape(TILE // 8, 8, ROWS), axis=0)

        total = jnp.zeros((8, ROWS), jnp.float32)
        if own:
            total = inner(edge, lax.fori_loop(0, edge, inner, total), True)
        else:
            for tile in range(TILES):
                total = inner(tile, total)
        return jnp.sum(total, axis=0, keepdims=True)

    def keep(k, level, total):
        level_ref[k] = level
        if not swapped:
            out_ref[y + k, 0:1, :] = level
            out_ref[y + k, 1:2, :] = total
            return
        first = given[0][y + k, 0:1, :]
        top = jnp.maximum(first, level)
        out_ref[y + k, 0:1, :] = top
        out_ref[y + k, 1:2, :] = given[0][y + k, 1:2, :] * jnp.exp2(first - top) + total * jnp.exp2(level - top)

    def quick(k, own):
        some = mxu(keys_ref[0, :TOK], qs[k], NT) * scale_of(k)
        if own:
            key = side * TOK + lax.broadcasted_iota(jnp.int32, (TOK, 1), 0)
            some = jnp.where(key <= local, some, MASKED)
        level = jnp.maximum(jnp.max(some, axis=0, keepdims=True), LOWEST)
        total = fill(k, own, level)
        keep(k, level, total)
        return jnp.max(total) > TOO_LARGE

    def careful(k, tiles, own):
        scale = scale_of(k)
        best_ref[...] = jnp.full((1, ROWS), LOWEST, jnp.float32)

        def inner(tile, unused):
            logits = mxu(rows_of(keys_ref, tile, 0), qs[k], NT) * scale
            if own:
                logits = jnp.where(visible(tile, side, local), logits, MASKED)
            best_ref[...] = jnp.maximum(best_ref[...], jnp.max(logits, axis=0, keepdims=True))
            return unused

        lax.fori_loop(0, tiles, inner, 0)
        level = best_ref[...]
        keep(k, level, fill(k, own, level))

    pl.when(quick(0, True))(lambda: careful(0, edge + 1, True))

    def later(k, unused):
        pl.when(quick(k, False))(lambda: careful(k, TILES, False))
        return unused

    lax.fori_loop(1, RING - y, later, 0)


def student_kernel(bm_ref, bo_ref, c0, c1, c2, c3, ct, bt, acc, sums, state):
    y, group, core, offset = place()
    last = RING - y
    below = (group * TOK, (group + core) * TOK)
    row_of = lax.broadcasted_iota(jnp.int32, (TILE, 1), 0)
    for k, c in enumerate((c0, c1, c2, c3)):
        for h in range(HEADS):
            ct[k, :, h * TOK:(h + 1) * TOK] = c[:, h * HEAD:(h + 1) * HEAD].T

    def shrink(k):
        pos = query_rows((y + k) * BLOCK + offset).astype(jnp.float32)
        return 1.0 / (math.sqrt(HEAD) * (pos + 1.0))

    def early(half, tile, bs):
        return jnp.where(row_of + tile * TILE < below[half], bs, jnp.zeros_like(bs))

    before = jnp.zeros((HEAD, HEAD), jnp.float32)
    whole = jnp.zeros((HEAD, HEAD), jnp.float32)
    for half, b_ref in enumerate((bm_ref, bo_ref)):
        for tile in range(TILES):
            bs = rows_of(b_ref, tile, TOK)
            turned = bs.T
            bt[half, :, tile * TILE:(tile + 1) * TILE] = turned
            before += mxu(turned, early(half, tile, bs), NN)
            whole += mxu(turned, bs, NN)

    def apply(square, k):
        high = narrow(square)
        low = narrow(square - high.astype(jnp.float32))
        return (mxu(high, ct[k], NN) + mxu(low, ct[k], NN)) * shrink(k)

    state[...] = jnp.zeros((HEAD, HEAD), jnp.float32)

    def later(k, unused):
        acc[k] = apply(whole, k)
        state[...] += mxu(narrow(ct[k].astype(jnp.float32) * shrink(k)), ct[k], NT)
        return unused

    lax.fori_loop(1, last, later, 0)
    own = mxu(narrow(ct[0].astype(jnp.float32) * shrink(0)), ct[0], NT)
    both = narrow(jnp.concatenate([state[...], own], axis=0))
    for half, b_ref in enumerate((bm_ref, bo_ref)):
        for tile in range(TILES):
            bs = rows_of(b_ref, tile, TOK)
            pair = jnp.concatenate([bs, early(half, tile, bs)], axis=1)
            sums[half, tile * TILE:(tile + 1) * TILE, :] = mxu(pair, both, NN)

    bs = bm_ref[group, TOK:]
    error = mxu(bs, ct[0], NN) * shrink(0)
    inside = lax.broadcasted_iota(jnp.int32, (TOK, 1), 0) <= query_rows(0)
    error = narrow(jnp.where(inside, error, 0.0))
    sums[0, pl.ds(pl.multiple_of(group * TOK, TOK), TOK), :] += mxu(error, ct[0], NT)
    acc[0] = apply(before, 0) + mxu(bs, error, TN)


def lse_of(stats, chunk):
    best = functools.reduce(jnp.maximum, [t[chunk, 0:1, :] for t in stats])
    total = sum(t[chunk, 1:2, :] * jnp.exp2(t[chunk, 0:1, :] - best) for t in stats)
    return best + jnp.log(total) * LOG2E


def key_sums_kernel(half, p_ref, level_ref, t0, t1, t2, t3, ct, sums_in, *refs):
    *received, g_ref, sums = refs
    y, group, _, _ = place()
    factor = LOSS_GAIN / math.sqrt(HEAD)
    sums[...] = sums_in[half]

    def weighted(k):
        fit = jnp.exp2(level_ref[k] - lse_of((t0, t1, t2, t3), y + k))
        return narrow(ct[k].astype(jnp.float32) * fit)

    own = weighted(0)

    def inner(tile, unused):
        rows = pl.ds(pl.multiple_of(tile * TILE, TILE), TILE)
        sums[rows, :] -= mxu(p_ref[0, rows, :], own, NT)
        return unused

    lax.fori_loop(0, group // PIECES + 1, inner, 0)

    def later(k, unused):
        sums[...] -= mxu(p_ref[k], weighted(k), NT)
        return unused

    lax.fori_loop(1, RING - y, later, 0)
    value = sums[...] * factor
    if received:
        value = value + received[0][...].astype(jnp.float32)
    g_ref[...] = narrow(value)


def row_sums_kernel(pm_ref, po_ref, lm_ref, lo_ref, t0, t1, t2, t3, bt, acc_in, o0, o1, o2, o3, acc):
    y, group, _, _ = place()
    factor = LOSS_GAIN / math.sqrt(HEAD)
    last = RING - y

    def fits(k):
        lse = lse_of((t0, t1, t2, t3), y + k)
        return jnp.exp2(lm_ref[k] - lse), jnp.exp2(lo_ref[k] - lse)

    fit = fits(0)
    acc[0] = acc_in[0]

    def inner(tile, unused):
        rows = pl.ds(pl.multiple_of(tile * TILE, TILE), TILE)
        acc[0] -= mxu(bt[0, :, rows], pm_ref[0, rows, :], NN) * fit[0]
        acc[0] -= mxu(bt[1, :, rows], po_ref[0, rows, :], NN) * fit[1]
        return unused

    lax.fori_loop(0, group // PIECES + 1, inner, 0)

    def later(k, unused):
        fit = fits(k)
        mine = mxu(bt[0], pm_ref[k], NN) * fit[0]
        other = mxu(bt[1], po_ref[k], NN) * fit[1]
        acc[k] = acc_in[k] - mine - other
        return unused

    lax.fori_loop(1, last, later, 0)

    for k, o in enumerate((o0, o1, o2, o3)):
        @pl.when(k < last)
        def _():
            for h in range(HEADS):
                piece = acc[k, :, h * TOK:(h + 1) * TOK].T * factor
                o[:, h * HEAD:(h + 1) * HEAD] = piece.astype(o.dtype)

        @pl.when(k >= last)
        def _():
            o[...] = jnp.zeros(o.shape, o.dtype)


def down(value, k):
    return lax.ppermute(value, "y", [(s, s - k) for s in range(k, RING)])


def up(value, k):
    return lax.ppermute(value, "y", [(s, s + k) for s in range(RING - k)])


def around(value, k):
    return lax.ppermute(value, "y", [(s, (s + k) % RING) for s in range(RING)])


def swap(value):
    return lax.ppermute(value, "c", [(0, 1), (1, 0)])


def exchange(value):
    return lax.all_to_all(value, PLANE, 0, 0, tiled=True)


def on_device(hidden_states, w_c, w_b, teacher_q, teacher_k):
    shaped = jax.ShapeDtypeStruct
    bf16 = jnp.bfloat16
    hbm, vmem = pl.BlockSpec(memory_space=pltpu.HBM), pl.BlockSpec(memory_space=pltpu.VMEM)
    limit = pltpu.CompilerParams(vmem_limit_bytes=VMEM_LIMIT)
    pairs = pl.pallas_call(
        project_b_kernel,
        out_shape=shaped((PLANE_N, 2 * TOK, HEAD), bf16),
        in_specs=[hbm, hbm, vmem],
        out_specs=hbm,
        scratch_shapes=[pltpu.VMEM(hidden_states.shape, bf16), pltpu.VMEM(w_b.shape, bf16), pltpu.VMEM((2 * TOK, HEAD), bf16),
                        pltpu.SemaphoreType.DMA((2 * DEPTH,)), pltpu.SemaphoreType.DMA((PLANE_N,))],
        compiler_params=pltpu.CompilerParams(vmem_limit_bytes=127 * 512 * 1024),
        name="project_b",
    )(hidden_states, w_b, teacher_k)
    mine = exchange(pairs)
    queries = [teacher_q] + [down(teacher_q, k) for k in (1, 2, 3)]
    c_proj = pl.pallas_call(
        project_c_kernel,
        out_shape=shaped((TOK, ROWS), bf16),
        in_specs=[hbm, hbm],
        out_specs=vmem,
        scratch_shapes=[pltpu.VMEM(hidden_states.shape, bf16), pltpu.VMEM(w_c.shape, bf16),
                        pltpu.SemaphoreType.DMA((2 * DEPTH,))],
        compiler_params=pltpu.CompilerParams(vmem_limit_bytes=58 * 1024 * 1024),
        name="project_c",
    )(hidden_states, w_c)
    crows = [c_proj] + [down(c_proj, k) for k in (1, 2, 3)]
    other = swap(mine)

    def call(kernel, ins, outs, scratch):
        return pl.pallas_call(
            kernel,
            out_shape=outs,
            in_specs=[vmem] * len(ins),
            out_specs=jax.tree.map(lambda unused: vmem, outs),
            scratch_shapes=[pltpu.VMEM(*s) for s in scratch],
            compiler_params=limit,
        )(*ins)

    full, half = jnp.float32, jnp.bfloat16
    kept = (shaped((RING, HALF, ROWS), half), shaped((RING, 1, ROWS), full), shaped((RING, 2, ROWS), full))
    room = [((RING, ROWS, HEAD), half), ((1, ROWS), full)]
    p_mine, l_mine, first = call(
        functools.partial(weights_kernel, False), (mine, *queries), kept, room)
    p_other, l_other, stats = call(
        functools.partial(weights_kernel, True), (other, *queries, first), kept, room)
    all_stats = [stats] + [around(stats, k) for k in (1, 2, 3)]
    ct, bt, acc, sums = call(
        student_kernel, (mine, other, *crows),
        (shaped((RING, HEAD, ROWS), half), shaped((2, HEAD, HALF), half),
         shaped((RING, HEAD, ROWS), full), shaped((2, HALF, HEAD), full)),
        [((HEAD, HEAD), full)],
    )
    held = [((HALF, HEAD), full)]
    g_other = call(functools.partial(key_sums_kernel, 1),
                   (p_other, l_other, *all_stats, ct, sums), shaped((HALF, HEAD), half), held)
    g_swapped = swap(g_other)
    part = shaped((TOK, ROWS), half)
    o0, o1, o2, o3 = call(
        row_sums_kernel, (p_mine, p_other, l_mine, l_other, *all_stats, bt, acc),
        (shaped((TOK, ROWS), full), part, part, part),
        [((RING, HEAD, ROWS), full)],
    )
    g_sum = call(functools.partial(key_sums_kernel, 0),
                 (p_mine, l_mine, *all_stats, ct, sums, g_swapped), shaped((HALF, HEAD), half), held)
    g_parts = exchange(g_sum.reshape(PLANE_N, TOK, HEAD))
    given = [up(o, k) for k, o in ((1, o1), (2, o2), (3, o3))]
    rows = o0 + sum(o.astype(full) for o in given)
    grad_b = jnp.sum(g_parts.astype(full), axis=0)
    return narrow(rows), narrow(grad_b)


def solution(mesh):
    inner = Mesh(mesh.devices.reshape(SIZES), AXES)
    tokens = P(AXES, None)

    return jax.shard_map(
        on_device,
        mesh=inner,
        in_specs=(tokens, P(), P(), tokens, tokens),
        out_specs=(tokens, tokens),
        check_vma=False,
    )
```

```python
import functools
import math

import jax
import jax.numpy as jnp
from jax import lax
from jax.experimental import pallas as pl
from jax.experimental.pallas import tpu as pltpu
from jax.sharding import Mesh, PartitionSpec as P


HEADS = 4
HEAD = 128
TOK = 128
LOSS_GAIN = 16.0
LENGTH_BASE = 512.0
LOG2E = math.log2(math.e)

AXES = ("y", "zl", "x", "zh", "c")
SIZES = (4, 2, 4, 2, 2)
PLANE = ("zl", "x", "zh")
PLANE_N = 16
RING = 4
HALF = PLANE_N * TOK
BLOCK = 2 * HALF
ROWS = HEADS * TOK
TILE = 1024
TILES = HALF // TILE
PIECES = TILE // TOK
DEPTH = 4
MASKED = -1e30
LOWEST = -1e29
TOO_LARGE = 2.0 ** 60
VMEM_LIMIT = 20 * 1024 * 1024


NT = (((1,), (1,)), ((), ()))
NN = (((1,), (0,)), ((), ()))
TN = (((0,), (0,)), ((), ()))


def mxu(a, b, dims):
    return lax.dot_general(a, b, dims, preferred_element_type=jnp.float32)


def stack_heads(dst, slot, src):
    for h in range(HEADS):
        dst[slot, h * TOK:(h + 1) * TOK, :] = src[:, h * HEAD:(h + 1) * HEAD]


def query_rows(first):
    lane = lax.broadcasted_iota(jnp.int32, (1, ROWS), 1)
    return first + (lane & (TOK - 1))


def temper(pos):
    scale = LOG2E / (math.log(LENGTH_BASE) * math.sqrt(HEAD))
    return jnp.log(pos.astype(jnp.float32) + 2.0) * scale


def visible(tile, core, query):
    row = lax.broadcasted_iota(jnp.int32, (TILE, 1), 0)
    group = tile * PIECES + (row >> 7)
    key = (group * 2 + core) * TOK + (row & (TOK - 1))
    return key <= query


def place():
    group = (lax.axis_index("zl") * 4 + lax.axis_index("x")) * 2 + lax.axis_index("zh")
    core = lax.axis_index("c")
    return lax.axis_index("y"), group, core, (group * 2 + core) * TOK


def fetch(pairs, sems):
    copies = []
    for j, (source, target, split) in enumerate(pairs):
        size = source.shape[split] // DEPTH
        for i in range(DEPTH):
            cut = (slice(None),) * split + (pl.ds(i * size, size),)
            copies.append(pltpu.make_async_copy(source.at[cut], target.at[cut], sems.at[j * DEPTH + i]))
    for i in range(DEPTH):
        for copy in copies[i::DEPTH]:
            copy.start()
    return copies


def project(hidden, weights, copies):
    size = hidden.shape[1] // DEPTH
    total = None
    for i in range(DEPTH):
        for copy in copies[i::DEPTH]:
            copy.wait()
        part = mxu(hidden[:, i * size:(i + 1) * size], weights[i * size:(i + 1) * size, :], NN)
        total = part if total is None else total + part
    return narrow(total)


def project_b_kernel(h_ref, w_ref, k_ref, out_ref, hidden, weights, pair, sems, out_sems):
    copies = fetch(((h_ref, hidden, 1), (w_ref, weights, 0)), sems)
    pair[:TOK] = k_ref[...]
    pair[TOK:] = project(hidden, weights, copies)
    copies = [pltpu.make_async_copy(pair, out_ref.at[i], out_sems.at[i]) for i in range(PLANE_N)]
    for copy in copies:
        copy.start()
    for copy in copies:
        copy.wait()


def project_c_kernel(h_ref, w_ref, out_ref, hidden, weights, sems):
    copies = fetch(((h_ref, hidden, 1), (w_ref, weights, 0)), sems)
    out_ref[...] = project(hidden, weights, copies)


def rows_of(ref, tile, first, tiles=1):
    rows = ref[pl.ds(tile * PIECES, tiles * PIECES), first:first + TOK]
    return rows.reshape(tiles * TILE, HEAD)


def narrow(value):
    return value.astype(jnp.bfloat16)


def weights_kernel(swapped, *refs):
    keys_ref, *q_refs = refs[:1 + RING]
    given = refs[1 + RING:-5] if swapped else ()
    p_ref, level_ref, out_ref, qs, best_ref = refs[-5:]
    y, group, core, offset = place()
    for k, q in enumerate(q_refs):
        stack_heads(qs, k, q)
    for k in range(RING):
        out_ref[k, 0:1, :] = jnp.full((1, ROWS), LOWEST, jnp.float32)
        out_ref[k, 1:2, :] = jnp.zeros((1, ROWS), jnp.float32)
    local = query_rows(offset)
    side = 1 - core if swapped else core
    edge = group // PIECES

    def scale_of(k):
        return temper(query_rows((y + k) * BLOCK + offset))

    def fill(k, own, level):
        scale = scale_of(k)

        def inner(tile, total, masked=False):
            row = pl.multiple_of(tile * TILE, TILE)
            weight = jnp.exp2(mxu(rows_of(keys_ref, tile, 0), qs[k], NT) * scale - level)
            if masked:
                weight = jnp.where(visible(tile, side, local), weight, 0.0)
            p_ref[k, pl.ds(row, TILE), :] = narrow(weight)
            return total + jnp.sum(weight.reshape(TILE // 8, 8, ROWS), axis=0)

        total = jnp.zeros((8, ROWS), jnp.float32)
        if own:
            total = inner(edge, lax.fori_loop(0, edge, inner, total), True)
        else:
            for tile in range(TILES):
                total = inner(tile, total)
        return jnp.sum(total, axis=0, keepdims=True)

    def keep(k, level, total):
        level_ref[k] = level
        if not swapped:
            out_ref[y + k, 0:1, :] = level
            out_ref[y + k, 1:2, :] = total
            return
        first = given[0][y + k, 0:1, :]
        top = jnp.maximum(first, level)
        out_ref[y + k, 0:1, :] = top
        out_ref[y + k, 1:2, :] = given[0][y + k, 1:2, :] * jnp.exp2(first - top) + total * jnp.exp2(level - top)

    def quick(k, own):
        some = mxu(keys_ref[0, :TOK], qs[k], NT) * scale_of(k)
        if own:
            key = side * TOK + lax.broadcasted_iota(jnp.int32, (TOK, 1), 0)
            some = jnp.where(key <= local, some, MASKED)
        level = jnp.maximum(jnp.max(some, axis=0, keepdims=True), LOWEST)
        total = fill(k, own, level)
        keep(k, level, total)
        return jnp.max(total) > TOO_LARGE

    def careful(k, tiles, own):
        scale = scale_of(k)
        best_ref[...] = jnp.full((1, ROWS), LOWEST, jnp.float32)

        def inner(tile, unused):
            logits = mxu(rows_of(keys_ref, tile, 0), qs[k], NT) * scale
            if own:
                logits = jnp.where(visible(tile, side, local), logits, MASKED)
            best_ref[...] = jnp.maximum(best_ref[...], jnp.max(logits, axis=0, keepdims=True))
            return unused

        lax.fori_loop(0, tiles, inner, 0)
        level = best_ref[...]
        keep(k, level, fill(k, own, level))

    pl.when(quick(0, True))(lambda: careful(0, edge + 1, True))

    def later(k, unused):
        pl.when(quick(k, False))(lambda: careful(k, TILES, False))
        return unused

    lax.fori_loop(1, RING - y, later, 0)


def student_kernel(bm_ref, bo_ref, c0, c1, c2, c3, ct, bt, acc, sums, state):
    y, group, core, offset = place()
    last = RING - y
    below = (group * TOK, (group + core) * TOK)
    row_of = lax.broadcasted_iota(jnp.int32, (TILE, 1), 0)
    for k, c in enumerate((c0, c1, c2, c3)):
        for h in range(HEADS):
            ct[k, :, h * TOK:(h + 1) * TOK] = c[:, h * HEAD:(h + 1) * HEAD].T

    def shrink(k):
        pos = query_rows((y + k) * BLOCK + offset).astype(jnp.float32)
        return 1.0 / (math.sqrt(HEAD) * (pos + 1.0))

    def early(half, tile, bs):
        return jnp.where(row_of + tile * TILE < below[half], bs, jnp.zeros_like(bs))

    before = jnp.zeros((HEAD, HEAD), jnp.float32)
    whole = jnp.zeros((HEAD, HEAD), jnp.float32)
    for half, b_ref in enumerate((bm_ref, bo_ref)):
        for tile in range(TILES):
            bs = rows_of(b_ref, tile, TOK)
            turned = bs.T
            bt[half, :, tile * TILE:(tile + 1) * TILE] = turned
            before += mxu(turned, early(half, tile, bs), NN)
            whole += mxu(turned, bs, NN)

    def apply(square, k):
        high = narrow(square)
        low = narrow(square - high.astype(jnp.float32))
        return (mxu(high, ct[k], NN) + mxu(low, ct[k], NN)) * shrink(k)

    state[...] = jnp.zeros((HEAD, HEAD), jnp.float32)

    def later(k, unused):
        acc[k] = apply(whole, k)
        state[...] += mxu(narrow(ct[k].astype(jnp.float32) * shrink(k)), ct[k], NT)
        return unused

    lax.fori_loop(1, last, later, 0)
    own = mxu(narrow(ct[0].astype(jnp.float32) * shrink(0)), ct[0], NT)
    both = narrow(jnp.concatenate([state[...], own], axis=0))
    for half, b_ref in enumerate((bm_ref, bo_ref)):
        for tile in range(TILES):
            bs = rows_of(b_ref, tile, TOK)
            pair = jnp.concatenate([bs, early(half, tile, bs)], axis=1)
            sums[half, tile * TILE:(tile + 1) * TILE, :] = mxu(pair, both, NN)

    bs = bm_ref[group, TOK:]
    error = mxu(bs, ct[0], NN) * shrink(0)
    inside = lax.broadcasted_iota(jnp.int32, (TOK, 1), 0) <= query_rows(0)
    error = narrow(jnp.where(inside, error, 0.0))
    sums[0, pl.ds(pl.multiple_of(group * TOK, TOK), TOK), :] += mxu(error, ct[0], NT)
    acc[0] = apply(before, 0) + mxu(bs, error, TN)


def lse_of(stats, chunk):
    best = functools.reduce(jnp.maximum, [t[chunk, 0:1, :] for t in stats])
    total = sum(t[chunk, 1:2, :] * jnp.exp2(t[chunk, 0:1, :] - best) for t in stats)
    return best + jnp.log(total) * LOG2E


def key_sums_kernel(half, p_ref, level_ref, t0, t1, t2, t3, ct, sums_in, *refs):
    spread = half == 0
    received = refs[0] if spread else None
    *spread_refs, sums = refs[1:] if spread else refs
    y, group, _, _ = place()
    factor = LOSS_GAIN / math.sqrt(HEAD)
    sums[...] = sums_in[half]

    def weighted(k):
        fit = jnp.exp2(level_ref[k] - lse_of((t0, t1, t2, t3), y + k))
        return narrow(ct[k].astype(jnp.float32) * fit)

    own = weighted(0)

    def inner(tile, unused):
        rows = pl.ds(pl.multiple_of(tile * TILE, TILE), TILE)
        sums[rows, :] -= mxu(p_ref[0, rows, :], own, NT)
        return unused

    lax.fori_loop(0, group // PIECES + 1, inner, 0)

    def later(k, unused):
        sums[...] -= mxu(p_ref[k], weighted(k), NT)
        return unused

    lax.fori_loop(1, RING - y, later, 0)
    if not spread:
        spread_refs[0][...] = narrow(sums[...] * factor)
        return
    x = lax.axis_index("x")
    for k, ref in enumerate(spread_refs):
        for z in range(RING):
            spot = (z // 2) * 2 * RING + ((x + k) & (RING - 1)) * 2 + z % 2
            rows = pl.ds(pl.multiple_of(spot * TOK, TOK), TOK)
            ref[z] = (sums[rows, :] * factor + received[rows, :].astype(jnp.float32)).astype(ref.dtype)


def join_x_kernel(own, r1, r2, r3, s0, s1, s2, s3, sums):
    total = own[...]
    for ref in (r1, r2, r3):
        total = total + ref[...].astype(jnp.float32)
    sums[...] = total
    z = lax.axis_index("zh") * 2 + lax.axis_index("zl")
    for k, ref in enumerate((s0, s1, s2, s3)):
        target = (z + k) & (RING - 1)
        ref[...] = sums[(target & 1) * 2 + (target >> 1)].astype(ref.dtype)


def row_sums_kernel(pm_ref, po_ref, lm_ref, lo_ref, t0, t1, t2, t3, bt, acc_in, o0, o1, o2, o3, acc):
    y, group, _, _ = place()
    factor = LOSS_GAIN / math.sqrt(HEAD)
    last = RING - y

    def fits(k):
        lse = lse_of((t0, t1, t2, t3), y + k)
        return jnp.exp2(lm_ref[k] - lse), jnp.exp2(lo_ref[k] - lse)

    fit = fits(0)
    acc[0] = acc_in[0]

    def inner(tile, unused):
        rows = pl.ds(pl.multiple_of(tile * TILE, TILE), TILE)
        acc[0] -= mxu(bt[0, :, rows], pm_ref[0, rows, :], NN) * fit[0]
        acc[0] -= mxu(bt[1, :, rows], po_ref[0, rows, :], NN) * fit[1]
        return unused

    lax.fori_loop(0, group // PIECES + 1, inner, 0)

    def later(k, unused):
        fit = fits(k)
        mine = mxu(bt[0], pm_ref[k], NN) * fit[0]
        other = mxu(bt[1], po_ref[k], NN) * fit[1]
        acc[k] = acc_in[k] - mine - other
        return unused

    lax.fori_loop(1, last, later, 0)

    for k, o in enumerate((o0, o1, o2, o3)):
        @pl.when(k < last)
        def _():
            for h in range(HEADS):
                piece = acc[k, :, h * TOK:(h + 1) * TOK].T * factor
                o[:, h * HEAD:(h + 1) * HEAD] = piece.astype(o.dtype)

        @pl.when(k >= last)
        def _():
            o[...] = jnp.zeros(o.shape, o.dtype)


def down(value, k):
    return lax.ppermute(value, "y", [(s, s - k) for s in range(k, RING)])


def up(value, k):
    return lax.ppermute(value, "y", [(s, s + k) for s in range(RING - k)])


def around(value, k):
    return lax.ppermute(value, "y", [(s, (s + k) % RING) for s in range(RING)])


def along_x(value, k):
    return lax.ppermute(value, "x", [(s, (s + k) % RING) for s in range(RING)])


def along_z(value, k):
    index = [(z % 2) * 2 + z // 2 for z in range(RING)]
    return lax.ppermute(value, ("zl", "zh"), [(index[z], index[(z + k) % RING]) for z in range(RING)])


def swap(value):
    return lax.ppermute(value, "c", [(0, 1), (1, 0)])


def exchange(value):
    return lax.all_to_all(value, PLANE, 0, 0, tiled=True)


def on_device(hidden_states, w_c, w_b, teacher_q, teacher_k):
    shaped = jax.ShapeDtypeStruct
    bf16 = jnp.bfloat16
    hbm, vmem = pl.BlockSpec(memory_space=pltpu.HBM), pl.BlockSpec(memory_space=pltpu.VMEM)
    limit = pltpu.CompilerParams(vmem_limit_bytes=VMEM_LIMIT)
    pairs = pl.pallas_call(
        project_b_kernel,
        out_shape=shaped((PLANE_N, 2 * TOK, HEAD), bf16),
        in_specs=[hbm, hbm, vmem],
        out_specs=hbm,
        scratch_shapes=[pltpu.VMEM(hidden_states.shape, bf16), pltpu.VMEM(w_b.shape, bf16), pltpu.VMEM((2 * TOK, HEAD), bf16),
                        pltpu.SemaphoreType.DMA((2 * DEPTH,)), pltpu.SemaphoreType.DMA((PLANE_N,))],
        compiler_params=pltpu.CompilerParams(vmem_limit_bytes=127 * 512 * 1024),
        name="project_b",
    )(hidden_states, w_b, teacher_k)
    mine = exchange(pairs)
    queries = [teacher_q] + [down(teacher_q, k) for k in (1, 2, 3)]
    c_proj = pl.pallas_call(
        project_c_kernel,
        out_shape=shaped((TOK, ROWS), bf16),
        in_specs=[hbm, hbm],
        out_specs=vmem,
        scratch_shapes=[pltpu.VMEM(hidden_states.shape, bf16), pltpu.VMEM(w_c.shape, bf16),
                        pltpu.SemaphoreType.DMA((2 * DEPTH,))],
        compiler_params=pltpu.CompilerParams(vmem_limit_bytes=58 * 1024 * 1024),
        name="project_c",
    )(hidden_states, w_c)
    crows = [c_proj] + [down(c_proj, k) for k in (1, 2, 3)]
    other = swap(mine)

    def call(kernel, ins, outs, scratch):
        return pl.pallas_call(
            kernel,
            out_shape=outs,
            in_specs=[vmem] * len(ins),
            out_specs=jax.tree.map(lambda unused: vmem, outs),
            scratch_shapes=[pltpu.VMEM(*s) for s in scratch],
            compiler_params=limit,
        )(*ins)

    full, half = jnp.float32, jnp.bfloat16
    kept = (shaped((RING, HALF, ROWS), half), shaped((RING, 1, ROWS), full), shaped((RING, 2, ROWS), full))
    room = [((RING, ROWS, HEAD), half), ((1, ROWS), full)]
    p_mine, l_mine, first = call(
        functools.partial(weights_kernel, False), (mine, *queries), kept, room)
    p_other, l_other, stats = call(
        functools.partial(weights_kernel, True), (other, *queries, first), kept, room)
    all_stats = [stats] + [around(stats, k) for k in (1, 2, 3)]
    ct, bt, acc, sums = call(
        student_kernel, (mine, other, *crows),
        (shaped((RING, HEAD, ROWS), half), shaped((2, HEAD, HALF), half),
         shaped((RING, HEAD, ROWS), full), shaped((2, HALF, HEAD), full)),
        [((HEAD, HEAD), full)],
    )
    held = [((HALF, HEAD), full)]
    g_other = call(functools.partial(key_sums_kernel, 1),
                   (p_other, l_other, *all_stats, ct, sums), shaped((HALF, HEAD), half), held)
    g_swapped = swap(g_other)
    sent = shaped((RING, TOK, HEAD), half)
    g0, *g_sent = call(
        functools.partial(key_sums_kernel, 0),
        (p_mine, l_mine, *all_stats, ct, sums, g_swapped),
        (shaped((RING, TOK, HEAD), full), sent, sent, sent), held)
    g_near = [along_x(g, k) for k, g in enumerate(g_sent, 1)]
    part = shaped((TOK, ROWS), half)
    o0, *o_sent = call(
        row_sums_kernel, (p_mine, p_other, l_mine, l_other, *all_stats, bt, acc),
        (shaped((TOK, ROWS), full), part, part, part),
        [((RING, HEAD, ROWS), full)],
    )
    given = [up(o, k) for k, o in enumerate(o_sent, 1)]
    sent = shaped((TOK, HEAD), half)
    h0, *h_sent = call(join_x_kernel, (g0, *g_near), (shaped((TOK, HEAD), full), sent, sent, sent),
                       [((RING, TOK, HEAD), full)])
    g_far = [along_z(h, k) for k, h in enumerate(h_sent, 1)]
    rows = o0 + sum(o.astype(full) for o in given)
    grad_b = h0 + sum(h.astype(full) for h in g_far)
    return narrow(rows), narrow(grad_b)


def solution(mesh):
    inner = Mesh(mesh.devices.reshape(SIZES), AXES)
    tokens = P(AXES, None)

    return jax.shard_map(
        on_device,
        mesh=inner,
        in_specs=(tokens, P(), P(), tokens, tokens),
        out_specs=(tokens, tokens),
        check_vma=False,
    )
```

```python
import functools
import math

import jax
import jax.numpy as jnp
from jax import lax
from jax.experimental import pallas as pl
from jax.experimental.pallas import tpu as pltpu
from jax.sharding import Mesh, PartitionSpec as P


HEADS = 4
HEAD = 128
TOK = 128
LOSS_GAIN = 16.0
LENGTH_BASE = 512.0
LOG2E = math.log2(math.e)

AXES = ("y", "zl", "x", "zh", "c")
SIZES = (4, 2, 4, 2, 2)
PLANE = ("zl", "x", "zh")
PLANE_N = 16
RING = 4
HALF = PLANE_N * TOK
BLOCK = 2 * HALF
ROWS = HEADS * TOK
TILE = 1024
TILES = HALF // TILE
PIECES = TILE // TOK
DEPTH = 4
MASKED = -1e30
LOWEST = -1e29
TOO_LARGE = 2.0 ** 60
VMEM_LIMIT = 20 * 1024 * 1024


NT = (((1,), (1,)), ((), ()))
NN = (((1,), (0,)), ((), ()))
TN = (((0,), (0,)), ((), ()))


def mxu(a, b, dims):
    return lax.dot_general(a, b, dims, preferred_element_type=jnp.float32)


def stack_heads(dst, slot, src):
    for h in range(HEADS):
        dst[slot, h * TOK:(h + 1) * TOK, :] = src[:, h * HEAD:(h + 1) * HEAD]


def query_rows(first):
    lane = lax.broadcasted_iota(jnp.int32, (1, ROWS), 1)
    return first + (lane & (TOK - 1))


def temper(pos):
    scale = LOG2E / (math.log(LENGTH_BASE) * math.sqrt(HEAD))
    return jnp.log(pos.astype(jnp.float32) + 2.0) * scale


def visible(tile, core, query):
    row = lax.broadcasted_iota(jnp.int32, (TILE, 1), 0)
    group = tile * PIECES + (row >> 7)
    key = (group * 2 + core) * TOK + (row & (TOK - 1))
    return key <= query


def place():
    group = (lax.axis_index("zl") * 4 + lax.axis_index("x")) * 2 + lax.axis_index("zh")
    core = lax.axis_index("c")
    return lax.axis_index("y"), group, core, (group * 2 + core) * TOK


def fetch(pairs, sems):
    copies = []
    for j, (source, target, split) in enumerate(pairs):
        size = source.shape[split] // DEPTH
        for i in range(DEPTH):
            cut = (slice(None),) * split + (pl.ds(i * size, size),)
            copies.append(pltpu.make_async_copy(source.at[cut], target.at[cut], sems.at[j * DEPTH + i]))
    for i in range(DEPTH):
        for copy in copies[i::DEPTH]:
            copy.start()
    return copies


def project(hidden, weights, copies):
    size = hidden.shape[1] // DEPTH
    total = None
    for i in range(DEPTH):
        for copy in copies[i::DEPTH]:
            copy.wait()
        part = mxu(hidden[:, i * size:(i + 1) * size], weights[i * size:(i + 1) * size, :], NN)
        total = part if total is None else total + part
    return narrow(total)


def project_b_kernel(h_ref, w_ref, k_ref, out_ref, hidden, weights, pair, sems, out_sems):
    copies = fetch(((h_ref, hidden, 1), (w_ref, weights, 0)), sems)
    pair[:TOK] = k_ref[...]
    pair[TOK:] = project(hidden, weights, copies)
    copies = [pltpu.make_async_copy(pair, out_ref.at[i], out_sems.at[i]) for i in range(PLANE_N)]
    for copy in copies:
        copy.start()
    for copy in copies:
        copy.wait()


def project_c_kernel(h_ref, w_ref, out_ref, hidden, weights, sems):
    copies = fetch(((h_ref, hidden, 1), (w_ref, weights, 0)), sems)
    out_ref[...] = project(hidden, weights, copies)


def rows_of(ref, tile, first, tiles=1):
    rows = ref[pl.ds(tile * PIECES, tiles * PIECES), first:first + TOK]
    return rows.reshape(tiles * TILE, HEAD)


def narrow(value):
    return value.astype(jnp.bfloat16)


def weights_kernel(swapped, *refs):
    keys_ref, *q_refs = refs[:1 + RING]
    given = refs[1 + RING:-5] if swapped else ()
    p_ref, level_ref, out_ref, qs, best_ref = refs[-5:]
    y, group, core, offset = place()
    for k, q in enumerate(q_refs):
        stack_heads(qs, k, q)
    for k in range(RING):
        out_ref[k, 0:1, :] = jnp.full((1, ROWS), LOWEST, jnp.float32)
        out_ref[k, 1:2, :] = jnp.zeros((1, ROWS), jnp.float32)
    local = query_rows(offset)
    side = 1 - core if swapped else core
    edge = group // PIECES

    def scale_of(k):
        return temper(query_rows((y + k) * BLOCK + offset))

    def fill(k, own, level):
        scale = scale_of(k)

        def inner(tile, total, masked=False):
            row = pl.multiple_of(tile * TILE, TILE)
            weight = jnp.exp2(mxu(rows_of(keys_ref, tile, 0), qs[k], NT) * scale - level)
            if masked:
                weight = jnp.where(visible(tile, side, local), weight, 0.0)
            p_ref[k, pl.ds(row, TILE), :] = narrow(weight)
            return total + jnp.sum(weight.reshape(TILE // 8, 8, ROWS), axis=0)

        total = jnp.zeros((8, ROWS), jnp.float32)
        if own:
            total = inner(edge, lax.fori_loop(0, edge, inner, total), True)
        else:
            for tile in range(TILES):
                total = inner(tile, total)
        return jnp.sum(total, axis=0, keepdims=True)

    def keep(k, level, total):
        level_ref[k] = level
        if not swapped:
            out_ref[y + k, 0:1, :] = level
            out_ref[y + k, 1:2, :] = total
            return
        first = given[0][y + k, 0:1, :]
        top = jnp.maximum(first, level)
        out_ref[y + k, 0:1, :] = top
        out_ref[y + k, 1:2, :] = given[0][y + k, 1:2, :] * jnp.exp2(first - top) + total * jnp.exp2(level - top)

    def quick(k, own):
        some = mxu(keys_ref[0, :TOK], qs[k], NT) * scale_of(k)
        if own:
            key = side * TOK + lax.broadcasted_iota(jnp.int32, (TOK, 1), 0)
            some = jnp.where(key <= local, some, MASKED)
        level = jnp.maximum(jnp.max(some, axis=0, keepdims=True), LOWEST)
        total = fill(k, own, level)
        keep(k, level, total)
        return jnp.max(total) > TOO_LARGE

    def careful(k, tiles, own):
        scale = scale_of(k)
        best_ref[...] = jnp.full((1, ROWS), LOWEST, jnp.float32)

        def inner(tile, unused):
            logits = mxu(rows_of(keys_ref, tile, 0), qs[k], NT) * scale
            if own:
                logits = jnp.where(visible(tile, side, local), logits, MASKED)
            best_ref[...] = jnp.maximum(best_ref[...], jnp.max(logits, axis=0, keepdims=True))
            return unused

        lax.fori_loop(0, tiles, inner, 0)
        level = best_ref[...]
        keep(k, level, fill(k, own, level))

    pl.when(quick(0, True))(lambda: careful(0, edge + 1, True))

    def later(k, unused):
        pl.when(quick(k, False))(lambda: careful(k, TILES, False))
        return unused

    lax.fori_loop(1, RING - y, later, 0)


def student_kernel(bm_ref, bo_ref, c0, c1, c2, c3, ct, bt, acc, sums, state):
    y, group, core, offset = place()
    last = RING - y
    below = (group * TOK, (group + core) * TOK)
    row_of = lax.broadcasted_iota(jnp.int32, (TILE, 1), 0)
    for k, c in enumerate((c0, c1, c2, c3)):
        for h in range(HEADS):
            ct[k, :, h * TOK:(h + 1) * TOK] = c[:, h * HEAD:(h + 1) * HEAD].T

    def shrink(k):
        pos = query_rows((y + k) * BLOCK + offset).astype(jnp.float32)
        return 1.0 / (math.sqrt(HEAD) * (pos + 1.0))

    def early(half, tile, bs):
        return jnp.where(row_of + tile * TILE < below[half], bs, jnp.zeros_like(bs))

    before = jnp.zeros((HEAD, HEAD), jnp.float32)
    whole = jnp.zeros((HEAD, HEAD), jnp.float32)
    for half, b_ref in enumerate((bm_ref, bo_ref)):
        for tile in range(TILES):
            bs = rows_of(b_ref, tile, TOK)
            turned = bs.T
            bt[half, :, tile * TILE:(tile + 1) * TILE] = turned
            before += mxu(turned, early(half, tile, bs), NN)
            whole += mxu(turned, bs, NN)

    def apply(square, k):
        high = narrow(square)
        low = narrow(square - high.astype(jnp.float32))
        return (mxu(high, ct[k], NN) + mxu(low, ct[k], NN)) * shrink(k)

    state[...] = jnp.zeros((HEAD, HEAD), jnp.float32)

    def later(k, unused):
        acc[k] = apply(whole, k)
        state[...] += mxu(narrow(ct[k].astype(jnp.float32) * shrink(k)), ct[k], NT)
        return unused

    lax.fori_loop(1, last, later, 0)
    own = mxu(narrow(ct[0].astype(jnp.float32) * shrink(0)), ct[0], NT)
    both = narrow(jnp.concatenate([state[...], own], axis=0))
    for half, b_ref in enumerate((bm_ref, bo_ref)):
        for tile in range(TILES):
            bs = rows_of(b_ref, tile, TOK)
            pair = jnp.concatenate([bs, early(half, tile, bs)], axis=1)
            sums[half, tile * TILE:(tile + 1) * TILE, :] = mxu(pair, both, NN)

    bs = bm_ref[group, TOK:]
    error = mxu(bs, ct[0], NN) * shrink(0)
    inside = lax.broadcasted_iota(jnp.int32, (TOK, 1), 0) <= query_rows(0)
    error = narrow(jnp.where(inside, error, 0.0))
    sums[0, pl.ds(pl.multiple_of(group * TOK, TOK), TOK), :] += mxu(error, ct[0], NT)
    acc[0] = apply(before, 0) + mxu(bs, error, TN)


def lse_of(stats, chunk):
    best = functools.reduce(jnp.maximum, [t[chunk, 0:1, :] for t in stats])
    total = sum(t[chunk, 1:2, :] * jnp.exp2(t[chunk, 0:1, :] - best) for t in stats)
    return best + jnp.log(total) * LOG2E


def key_sums_kernel(half, p_ref, level_ref, t0, t1, t2, t3, ct, sums_in, *refs):
    spread = half == 0
    received = refs[0] if spread else None
    *spread_refs, sums = refs[1:] if spread else refs
    y, group, _, _ = place()
    factor = LOSS_GAIN / math.sqrt(HEAD)
    sums[...] = sums_in[half]

    def weighted(k):
        fit = jnp.exp2(level_ref[k] - lse_of((t0, t1, t2, t3), y + k))
        return narrow(ct[k].astype(jnp.float32) * fit)

    own = weighted(0)

    def inner(tile, unused):
        rows = pl.ds(pl.multiple_of(tile * TILE, TILE), TILE)
        sums[rows, :] -= mxu(p_ref[0, rows, :], own, NT)
        return unused

    lax.fori_loop(0, group // PIECES + 1, inner, 0)

    def later(k, unused):
        sums[...] -= mxu(p_ref[k], weighted(k), NT)
        return unused

    lax.fori_loop(1, RING - y, later, 0)
    if not spread:
        spread_refs[0][...] = narrow(sums[...] * factor)
        return
    x = lax.axis_index("x")
    for k, ref in enumerate(spread_refs):
        for z in range(RING):
            spot = (z // 2) * 2 * RING + ((x + k) & (RING - 1)) * 2 + z % 2
            rows = pl.ds(pl.multiple_of(spot * TOK, TOK), TOK)
            ref[z] = (sums[rows, :] * factor + received[rows, :].astype(jnp.float32)).astype(ref.dtype)


def join_x_kernel(own, r1, r2, r3, s0, s1, s2, s3, sums):
    total = own[...]
    for ref in (r1, r2, r3):
        total = total + ref[...].astype(jnp.float32)
    sums[...] = total
    z = lax.axis_index("zh") * 2 + lax.axis_index("zl")
    for k, ref in enumerate((s0, s1, s2, s3)):
        target = (z + k) & (RING - 1)
        ref[...] = sums[(target & 1) * 2 + (target >> 1)].astype(ref.dtype)


def row_sums_kernel(early, pm_ref, po_ref, lm_ref, lo_ref, t0, t1, t2, t3, bt, acc_in, *refs):
    *outs, acc = refs
    y, group, _, _ = place()
    factor = LOSS_GAIN / math.sqrt(HEAD)
    last = RING - y

    def fits(k):
        lse = lse_of((t0, t1, t2, t3), y + k)
        return jnp.exp2(lm_ref[k] - lse), jnp.exp2(lo_ref[k] - lse)

    def whole(k):
        fit = fits(k)
        mine = mxu(bt[0], pm_ref[k], NN) * fit[0]
        other = mxu(bt[1], po_ref[k], NN) * fit[1]
        return acc_in[k] - mine - other

    def give(o, value):
        for h in range(HEADS):
            o[:, h * HEAD:(h + 1) * HEAD] = (value[:, h * TOK:(h + 1) * TOK].T * factor).astype(o.dtype)

    def later(k, o):
        @pl.when(k < last)
        def _():
            give(o, whole(k))

        @pl.when(k >= last)
        def _():
            o[...] = jnp.zeros(o.shape, o.dtype)

    if early:
        later(3, outs[0])
        later(2, outs[1])
        return
    later(1, outs[1])
    fit = fits(0)
    acc[...] = acc_in[0]

    def inner(tile, unused):
        rows = pl.ds(pl.multiple_of(tile * TILE, TILE), TILE)
        acc[...] -= mxu(bt[0, :, rows], pm_ref[0, rows, :], NN) * fit[0]
        acc[...] -= mxu(bt[1, :, rows], po_ref[0, rows, :], NN) * fit[1]
        return unused

    lax.fori_loop(0, group // PIECES + 1, inner, 0)
    give(outs[0], acc[...])


def down(value, k):
    return lax.ppermute(value, "y", [(s, s - k) for s in range(k, RING)])


def up(value, k):
    return lax.ppermute(value, "y", [(s, s + k) for s in range(RING - k)])


def around(value, k):
    return lax.ppermute(value, "y", [(s, (s + k) % RING) for s in range(RING)])


def along_x(value, k):
    return lax.ppermute(value, "x", [(s, (s + k) % RING) for s in range(RING)])


def along_z(value, k):
    index = [(z % 2) * 2 + z // 2 for z in range(RING)]
    return lax.ppermute(value, ("zl", "zh"), [(index[z], index[(z + k) % RING]) for z in range(RING)])


def swap(value):
    return lax.ppermute(value, "c", [(0, 1), (1, 0)])


def exchange(value):
    return lax.all_to_all(value, PLANE, 0, 0, tiled=True)


def on_device(hidden_states, w_c, w_b, teacher_q, teacher_k):
    shaped = jax.ShapeDtypeStruct
    bf16 = jnp.bfloat16
    hbm, vmem = pl.BlockSpec(memory_space=pltpu.HBM), pl.BlockSpec(memory_space=pltpu.VMEM)
    limit = pltpu.CompilerParams(vmem_limit_bytes=VMEM_LIMIT)
    pairs = pl.pallas_call(
        project_b_kernel,
        out_shape=shaped((PLANE_N, 2 * TOK, HEAD), bf16),
        in_specs=[hbm, hbm, vmem],
        out_specs=hbm,
        scratch_shapes=[pltpu.VMEM(hidden_states.shape, bf16), pltpu.VMEM(w_b.shape, bf16), pltpu.VMEM((2 * TOK, HEAD), bf16),
                        pltpu.SemaphoreType.DMA((2 * DEPTH,)), pltpu.SemaphoreType.DMA((PLANE_N,))],
        compiler_params=pltpu.CompilerParams(vmem_limit_bytes=127 * 512 * 1024),
        name="project_b",
    )(hidden_states, w_b, teacher_k)
    mine = exchange(pairs)
    queries = [teacher_q] + [down(teacher_q, k) for k in (1, 2, 3)]
    c_proj = pl.pallas_call(
        project_c_kernel,
        out_shape=shaped((TOK, ROWS), bf16),
        in_specs=[hbm, hbm],
        out_specs=vmem,
        scratch_shapes=[pltpu.VMEM(hidden_states.shape, bf16), pltpu.VMEM(w_c.shape, bf16),
                        pltpu.SemaphoreType.DMA((2 * DEPTH,))],
        compiler_params=pltpu.CompilerParams(vmem_limit_bytes=58 * 1024 * 1024),
        name="project_c",
    )(hidden_states, w_c)
    crows = [c_proj] + [down(c_proj, k) for k in (1, 2, 3)]
    other = swap(mine)

    def call(kernel, ins, outs, scratch):
        return pl.pallas_call(
            kernel,
            out_shape=outs,
            in_specs=[vmem] * len(ins),
            out_specs=jax.tree.map(lambda unused: vmem, outs),
            scratch_shapes=[pltpu.VMEM(*s) for s in scratch],
            compiler_params=limit,
        )(*ins)

    full, half = jnp.float32, jnp.bfloat16
    kept = (shaped((RING, HALF, ROWS), half), shaped((RING, 1, ROWS), full), shaped((RING, 2, ROWS), full))
    room = [((RING, ROWS, HEAD), half), ((1, ROWS), full)]
    p_mine, l_mine, first = call(
        functools.partial(weights_kernel, False), (mine, *queries), kept, room)
    p_other, l_other, stats = call(
        functools.partial(weights_kernel, True), (other, *queries, first), kept, room)
    all_stats = [stats] + [around(stats, k) for k in (1, 2, 3)]
    ct, bt, acc, sums = call(
        student_kernel, (mine, other, *crows),
        (shaped((RING, HEAD, ROWS), half), shaped((2, HEAD, HALF), half),
         shaped((RING, HEAD, ROWS), full), shaped((2, HALF, HEAD), full)),
        [((HEAD, HEAD), full)],
    )
    held = [((HALF, HEAD), full)]
    g_other = call(functools.partial(key_sums_kernel, 1),
                   (p_other, l_other, *all_stats, ct, sums), shaped((HALF, HEAD), half), held)
    g_swapped = swap(g_other)
    sent = shaped((RING, TOK, HEAD), half)
    g0, *g_sent = call(
        functools.partial(key_sums_kernel, 0),
        (p_mine, l_mine, *all_stats, ct, sums, g_swapped),
        (shaped((RING, TOK, HEAD), full), sent, sent, sent), held)
    g_near = [along_x(g, k) for k, g in enumerate(g_sent, 1)]
    part = shaped((TOK, ROWS), half)
    row_ins = (p_mine, p_other, l_mine, l_other, *all_stats, bt, acc)
    row_room = [((HEAD, ROWS), full)]
    o3, o2 = call(functools.partial(row_sums_kernel, True), row_ins, (part, part), row_room)
    o0, o1 = call(functools.partial(row_sums_kernel, False), row_ins,
                  (shaped((TOK, ROWS), full), part), row_room)
    given = [up(o, k) for k, o in enumerate((o1, o2, o3), 1)]
    sent = shaped((TOK, HEAD), half)
    h0, *h_sent = call(join_x_kernel, (g0, *g_near), (shaped((TOK, HEAD), full), sent, sent, sent),
                       [((RING, TOK, HEAD), full)])
    g_far = [along_z(h, k) for k, h in enumerate(h_sent, 1)]
    rows = o0 + sum(o.astype(full) for o in given)
    grad_b = h0 + sum(h.astype(full) for h in g_far)
    return narrow(rows), narrow(grad_b)


def solution(mesh):
    inner = Mesh(mesh.devices.reshape(SIZES), AXES)
    tokens = P(AXES, None)

    return jax.shard_map(
        on_device,
        mesh=inner,
        in_specs=(tokens, P(), P(), tokens, tokens),
        out_specs=(tokens, tokens),
        check_vma=False,
    )
```

```python
import functools
import math

import jax
import jax.numpy as jnp
from jax import lax
from jax.experimental import pallas as pl
from jax.experimental.pallas import tpu as pltpu
from jax.sharding import Mesh, PartitionSpec as P


HEADS = 4
HEAD = 128
TOK = 128
LOSS_GAIN = 16.0
LENGTH_BASE = 512.0
LOG2E = math.log2(math.e)

AXES = ("y", "zl", "x", "zh", "c")
SIZES = (4, 2, 4, 2, 2)
PLANE = ("zl", "x", "zh")
PLANE_N = 16
RING = 4
HALF = PLANE_N * TOK
BLOCK = 2 * HALF
ROWS = HEADS * TOK
TILE = 1024
TILES = HALF // TILE
PIECES = TILE // TOK
DEPTH = 4
MASKED = -1e30
LOWEST = -1e29
TOO_LARGE = 2.0 ** 60
VMEM_LIMIT = 20 * 1024 * 1024


NT = (((1,), (1,)), ((), ()))
NN = (((1,), (0,)), ((), ()))
TN = (((0,), (0,)), ((), ()))


def mxu(a, b, dims):
    return lax.dot_general(a, b, dims, preferred_element_type=jnp.float32)


def stack_heads(dst, slot, src):
    for h in range(HEADS):
        dst[slot, h * TOK:(h + 1) * TOK, :] = src[:, h * HEAD:(h + 1) * HEAD]


def query_rows(first):
    lane = lax.broadcasted_iota(jnp.int32, (1, ROWS), 1)
    return first + (lane & (TOK - 1))


def temper(pos):
    scale = LOG2E / (math.log(LENGTH_BASE) * math.sqrt(HEAD))
    return jnp.log(pos.astype(jnp.float32) + 2.0) * scale


def visible(tile, core, query):
    row = lax.broadcasted_iota(jnp.int32, (TILE, 1), 0)
    group = tile * PIECES + (row >> 7)
    key = (group * 2 + core) * TOK + (row & (TOK - 1))
    return key <= query


def place():
    group = (lax.axis_index("zl") * 4 + lax.axis_index("x")) * 2 + lax.axis_index("zh")
    core = lax.axis_index("c")
    return lax.axis_index("y"), group, core, (group * 2 + core) * TOK


def fetch(pairs, sems):
    copies = []
    for j, (source, target, split) in enumerate(pairs):
        size = source.shape[split] // DEPTH
        for i in range(DEPTH):
            cut = (slice(None),) * split + (pl.ds(i * size, size),)
            copies.append(pltpu.make_async_copy(source.at[cut], target.at[cut], sems.at[j * DEPTH + i]))
    for i in range(DEPTH):
        for copy in copies[i::DEPTH]:
            copy.start()
    return copies


def project(hidden, weights, copies):
    size = hidden.shape[1] // DEPTH
    total = None
    for i in range(DEPTH):
        for copy in copies[i::DEPTH]:
            copy.wait()
        part = mxu(hidden[:, i * size:(i + 1) * size], weights[i * size:(i + 1) * size, :], NN)
        total = part if total is None else total + part
    return narrow(total)


def project_b_kernel(h_ref, w_ref, k_ref, out_ref, hidden, weights, pair, sems, out_sems):
    copies = fetch(((h_ref, hidden, 1), (w_ref, weights, 0)), sems)
    pair[:TOK] = k_ref[...]
    pair[TOK:] = project(hidden, weights, copies)
    copies = [pltpu.make_async_copy(pair, out_ref.at[i], out_sems.at[i]) for i in range(PLANE_N)]
    for copy in copies:
        copy.start()
    for copy in copies:
        copy.wait()


def project_c_kernel(h_ref, w_ref, out_ref, hidden, weights, sems):
    copies = fetch(((h_ref, hidden, 1), (w_ref, weights, 0)), sems)
    out_ref[...] = project(hidden, weights, copies)


def rows_of(ref, tile, first, tiles=1):
    rows = ref[pl.ds(tile * PIECES, tiles * PIECES), first:first + TOK]
    return rows.reshape(tiles * TILE, HEAD)


def narrow(value):
    return value.astype(jnp.bfloat16)


def weights_kernel(swapped, *refs):
    keys_ref, *q_refs = refs[:1 + RING]
    given = refs[1 + RING:-5] if swapped else ()
    p_ref, level_ref, out_ref, qs, best_ref = refs[-5:]
    y, group, core, offset = place()
    for k, q in enumerate(q_refs):
        stack_heads(qs, k, q)
    for k in range(RING):
        out_ref[k, 0:1, :] = jnp.full((1, ROWS), LOWEST, jnp.float32)
        out_ref[k, 1:2, :] = jnp.zeros((1, ROWS), jnp.float32)
    local = query_rows(offset)
    side = 1 - core if swapped else core
    edge = group // PIECES

    def scale_of(k):
        return temper(query_rows((y + k) * BLOCK + offset))

    def fill(k, own, level):
        scale = scale_of(k)

        def inner(tile, total, masked=False):
            row = pl.multiple_of(tile * TILE, TILE)
            weight = jnp.exp2(mxu(rows_of(keys_ref, tile, 0), qs[k], NT) * scale - level)
            if masked:
                weight = jnp.where(visible(tile, side, local), weight, 0.0)
            p_ref[k, pl.ds(row, TILE), :] = narrow(weight)
            return total + jnp.sum(weight.reshape(TILE // 8, 8, ROWS), axis=0)

        total = jnp.zeros((8, ROWS), jnp.float32)
        if own:
            total = inner(edge, lax.fori_loop(0, edge, inner, total), True)
        else:
            for tile in range(TILES):
                total = inner(tile, total)
        return jnp.sum(total, axis=0, keepdims=True)

    def keep(k, level, total):
        level_ref[k] = level
        if not swapped:
            out_ref[y + k, 0:1, :] = level
            out_ref[y + k, 1:2, :] = total
            return
        first = given[0][y + k, 0:1, :]
        top = jnp.maximum(first, level)
        out_ref[y + k, 0:1, :] = top
        out_ref[y + k, 1:2, :] = given[0][y + k, 1:2, :] * jnp.exp2(first - top) + total * jnp.exp2(level - top)

    def quick(k, own):
        some = mxu(keys_ref[0, :TOK], qs[k], NT) * scale_of(k)
        if own:
            key = side * TOK + lax.broadcasted_iota(jnp.int32, (TOK, 1), 0)
            some = jnp.where(key <= local, some, MASKED)
        level = jnp.maximum(jnp.max(some, axis=0, keepdims=True), LOWEST)
        total = fill(k, own, level)
        keep(k, level, total)
        return jnp.max(total) > TOO_LARGE

    def careful(k, tiles, own):
        scale = scale_of(k)
        best_ref[...] = jnp.full((1, ROWS), LOWEST, jnp.float32)

        def inner(tile, unused):
            logits = mxu(rows_of(keys_ref, tile, 0), qs[k], NT) * scale
            if own:
                logits = jnp.where(visible(tile, side, local), logits, MASKED)
            best_ref[...] = jnp.maximum(best_ref[...], jnp.max(logits, axis=0, keepdims=True))
            return unused

        lax.fori_loop(0, tiles, inner, 0)
        level = best_ref[...]
        keep(k, level, fill(k, own, level))

    pl.when(quick(0, True))(lambda: careful(0, edge + 1, True))

    def later(k, unused):
        pl.when(quick(k, False))(lambda: careful(k, TILES, False))
        return unused

    lax.fori_loop(1, RING - y, later, 0)


def student_kernel(bm_ref, bo_ref, c0, c1, c2, c3, ct, bt, acc, sums, state):
    y, group, core, offset = place()
    last = RING - y
    below = (group * TOK, (group + core) * TOK)
    row_of = lax.broadcasted_iota(jnp.int32, (TILE, 1), 0)
    for k, c in enumerate((c0, c1, c2, c3)):
        for h in range(HEADS):
            ct[k, :, h * TOK:(h + 1) * TOK] = c[:, h * HEAD:(h + 1) * HEAD].T

    def shrink(k):
        pos = query_rows((y + k) * BLOCK + offset).astype(jnp.float32)
        return 1.0 / (math.sqrt(HEAD) * (pos + 1.0))

    def early(half, tile, bs):
        return jnp.where(row_of + tile * TILE < below[half], bs, jnp.zeros_like(bs))

    before = jnp.zeros((HEAD, HEAD), jnp.float32)
    whole = jnp.zeros((HEAD, HEAD), jnp.float32)
    for half, b_ref in enumerate((bm_ref, bo_ref)):
        for tile in range(TILES):
            bs = rows_of(b_ref, tile, TOK)
            turned = bs.T
            bt[half, :, tile * TILE:(tile + 1) * TILE] = turned
            before += mxu(turned, early(half, tile, bs), NN)
            whole += mxu(turned, bs, NN)

    def apply(square, k):
        high = narrow(square)
        low = narrow(square - high.astype(jnp.float32))
        return (mxu(high, ct[k], NN) + mxu(low, ct[k], NN)) * shrink(k)

    state[...] = jnp.zeros((HEAD, HEAD), jnp.float32)

    def later(k, unused):
        acc[k] = apply(whole, k)
        state[...] += mxu(narrow(ct[k].astype(jnp.float32) * shrink(k)), ct[k], NT)
        return unused

    lax.fori_loop(1, last, later, 0)
    own = mxu(narrow(ct[0].astype(jnp.float32) * shrink(0)), ct[0], NT)
    both = narrow(jnp.concatenate([state[...], own], axis=0))
    for half, b_ref in enumerate((bm_ref, bo_ref)):
        for tile in range(TILES):
            bs = rows_of(b_ref, tile, TOK)
            pair = jnp.concatenate([bs, early(half, tile, bs)], axis=1)
            sums[half, tile * TILE:(tile + 1) * TILE, :] = mxu(pair, both, NN)

    bs = bm_ref[group, TOK:]
    error = mxu(bs, ct[0], NN) * shrink(0)
    inside = lax.broadcasted_iota(jnp.int32, (TOK, 1), 0) <= query_rows(0)
    error = narrow(jnp.where(inside, error, 0.0))
    sums[0, pl.ds(pl.multiple_of(group * TOK, TOK), TOK), :] += mxu(error, ct[0], NT)
    acc[0] = apply(before, 0) + mxu(bs, error, TN)


def lse_of(stats, chunk):
    best = functools.reduce(jnp.maximum, [t[chunk, 0:1, :] for t in stats])
    total = sum(t[chunk, 1:2, :] * jnp.exp2(t[chunk, 0:1, :] - best) for t in stats)
    return best + jnp.log(total) * LOG2E


def key_sums_kernel(half, p_ref, level_ref, t0, t1, t2, t3, ct, sums_in, *refs):
    spread = half == 0
    received = refs[0] if spread else None
    *spread_refs, sums = refs[1:] if spread else refs
    y, group, _, _ = place()
    factor = LOSS_GAIN / math.sqrt(HEAD)
    sums[...] = sums_in[half]

    def weighted(k):
        fit = jnp.exp2(level_ref[k] - lse_of((t0, t1, t2, t3), y + k))
        return narrow(ct[k].astype(jnp.float32) * fit)

    own = weighted(0)

    def inner(tile, unused):
        rows = pl.ds(pl.multiple_of(tile * TILE, TILE), TILE)
        sums[rows, :] -= mxu(p_ref[0, rows, :], own, NT)
        return unused

    lax.fori_loop(0, group // PIECES + 1, inner, 0)

    def later(k, unused):
        sums[...] -= mxu(p_ref[k], weighted(k), NT)
        return unused

    lax.fori_loop(1, RING - y, later, 0)
    if not spread:
        spread_refs[0][...] = narrow(sums[...] * factor)
        return
    x = lax.axis_index("x")
    for k, ref in enumerate(spread_refs):
        for z in range(RING):
            spot = (z // 2) * 2 * RING + ((x + k) & (RING - 1)) * 2 + z % 2
            rows = pl.ds(pl.multiple_of(spot * TOK, TOK), TOK)
            ref[z] = (sums[rows, :] * factor + received[rows, :].astype(jnp.float32)).astype(ref.dtype)


def join_x_kernel(own, r1, r2, r3, s0, s1, s2, s3, sums):
    total = own[...]
    for ref in (r1, r2, r3):
        total = total + ref[...].astype(jnp.float32)
    sums[...] = total
    z = lax.axis_index("zh") * 2 + lax.axis_index("zl")
    for k, ref in enumerate((s0, s1, s2, s3)):
        target = (z + k) & (RING - 1)
        ref[...] = sums[(target & 1) * 2 + (target >> 1)].astype(ref.dtype)


def row_sums_kernel(early, pm_ref, po_ref, lm_ref, lo_ref, t0, t1, t2, t3, bt, acc_in, *refs):
    *outs, acc = refs
    y, group, _, _ = place()
    factor = LOSS_GAIN / math.sqrt(HEAD)
    last = RING - y

    def fits(k):
        lse = lse_of((t0, t1, t2, t3), y + k)
        return jnp.exp2(lm_ref[k] - lse), jnp.exp2(lo_ref[k] - lse)

    def whole(k):
        fit = fits(k)
        mine = mxu(bt[0], pm_ref[k], NN) * fit[0]
        other = mxu(bt[1], po_ref[k], NN) * fit[1]
        return acc_in[k] - mine - other

    def give(o, value):
        for h in range(HEADS):
            o[:, h * HEAD:(h + 1) * HEAD] = (value[:, h * TOK:(h + 1) * TOK].T * factor).astype(o.dtype)

    def later(k, o):
        @pl.when(k < last)
        def _():
            give(o, whole(k))

        @pl.when(k >= last)
        def _():
            o[...] = jnp.zeros(o.shape, o.dtype)

    if early:
        later(3, outs[0])
        later(2, outs[1])
        return
    later(1, outs[1])
    fit = fits(0)
    acc[...] = acc_in[0]

    def inner(tile, unused):
        rows = pl.ds(pl.multiple_of(tile * TILE, TILE), TILE)
        acc[...] -= mxu(bt[0, :, rows], pm_ref[0, rows, :], NN) * fit[0]
        acc[...] -= mxu(bt[1, :, rows], po_ref[0, rows, :], NN) * fit[1]
        return unused

    lax.fori_loop(0, group // PIECES + 1, inner, 0)
    give(outs[0], acc[...])


def down(value, k):
    return lax.ppermute(value, "y", [(s, s - k) for s in range(k, RING)])


def up(value, k):
    return lax.ppermute(value, "y", [(s, s + k) for s in range(RING - k)])


def around(value, k):
    return lax.ppermute(value, "y", [(s, (s + k) % RING) for s in range(RING)])


def along_x(value, k):
    return lax.ppermute(value, "x", [(s, (s + k) % RING) for s in range(RING)])


def along_z(value, k):
    index = [(z % 2) * 2 + z // 2 for z in range(RING)]
    return lax.ppermute(value, ("zl", "zh"), [(index[z], index[(z + k) % RING]) for z in range(RING)])


def swap(value):
    return lax.ppermute(value, "c", [(0, 1), (1, 0)])


def exchange(value):
    return lax.all_to_all(value, PLANE, 0, 0, tiled=True)


def on_device(hidden_states, w_c, w_b, teacher_q, teacher_k):
    shaped = jax.ShapeDtypeStruct
    bf16 = jnp.bfloat16
    hbm, vmem = pl.BlockSpec(memory_space=pltpu.HBM), pl.BlockSpec(memory_space=pltpu.VMEM)
    limit = pltpu.CompilerParams(vmem_limit_bytes=VMEM_LIMIT)
    pairs = pl.pallas_call(
        project_b_kernel,
        out_shape=shaped((PLANE_N, 2 * TOK, HEAD), bf16),
        in_specs=[hbm, hbm, vmem],
        out_specs=hbm,
        scratch_shapes=[pltpu.VMEM(hidden_states.shape, bf16), pltpu.VMEM(w_b.shape, bf16), pltpu.VMEM((2 * TOK, HEAD), bf16),
                        pltpu.SemaphoreType.DMA((2 * DEPTH,)), pltpu.SemaphoreType.DMA((PLANE_N,))],
        compiler_params=pltpu.CompilerParams(vmem_limit_bytes=127 * 512 * 1024),
        name="project_b",
    )(hidden_states, w_b, teacher_k)
    mine = exchange(pairs)
    queries = [teacher_q] + [down(teacher_q, k) for k in (1, 2, 3)]
    c_proj = pl.pallas_call(
        project_c_kernel,
        out_shape=shaped((TOK, ROWS), bf16),
        in_specs=[hbm, hbm],
        out_specs=vmem,
        scratch_shapes=[pltpu.VMEM(hidden_states.shape, bf16), pltpu.VMEM(w_c.shape, bf16),
                        pltpu.SemaphoreType.DMA((2 * DEPTH,))],
        compiler_params=pltpu.CompilerParams(vmem_limit_bytes=52 * 1024 * 1024),
        name="project_c",
    )(hidden_states, w_c)
    crows = [c_proj] + [down(c_proj, k) for k in (1, 2, 3)]
    other = swap(mine)

    def call(kernel, ins, outs, scratch):
        return pl.pallas_call(
            kernel,
            out_shape=outs,
            in_specs=[vmem] * len(ins),
            out_specs=jax.tree.map(lambda unused: vmem, outs),
            scratch_shapes=[pltpu.VMEM(*s) for s in scratch],
            compiler_params=limit,
        )(*ins)

    full, half = jnp.float32, jnp.bfloat16
    kept = (shaped((RING, HALF, ROWS), half), shaped((RING, 1, ROWS), full), shaped((RING, 2, ROWS), full))
    room = [((RING, ROWS, HEAD), half), ((1, ROWS), full)]
    p_mine, l_mine, first = call(
        functools.partial(weights_kernel, False), (mine, *queries), kept, room)
    p_other, l_other, stats = call(
        functools.partial(weights_kernel, True), (other, *queries, first), kept, room)
    all_stats = [stats] + [around(stats, k) for k in (1, 2, 3)]
    ct, bt, acc, sums = call(
        student_kernel, (mine, other, *crows),
        (shaped((RING, HEAD, ROWS), half), shaped((2, HEAD, HALF), half),
         shaped((RING, HEAD, ROWS), full), shaped((2, HALF, HEAD), full)),
        [((HEAD, HEAD), full)],
    )
    held = [((HALF, HEAD), full)]
    g_other = call(functools.partial(key_sums_kernel, 1),
                   (p_other, l_other, *all_stats, ct, sums), shaped((HALF, HEAD), half), held)
    g_swapped = swap(g_other)
    sent = shaped((RING, TOK, HEAD), half)
    g0, *g_sent = call(
        functools.partial(key_sums_kernel, 0),
        (p_mine, l_mine, *all_stats, ct, sums, g_swapped),
        (shaped((RING, TOK, HEAD), full), sent, sent, sent), held)
    g_near = [along_x(g, k) for k, g in enumerate(g_sent, 1)]
    part = shaped((TOK, ROWS), half)
    row_ins = (p_mine, p_other, l_mine, l_other, *all_stats, bt, acc)
    row_room = [((HEAD, ROWS), full)]
    o3, o2 = call(functools.partial(row_sums_kernel, True), row_ins, (part, part), row_room)
    o0, o1 = call(functools.partial(row_sums_kernel, False), row_ins,
                  (shaped((TOK, ROWS), full), part), row_room)
    given = [up(o, k) for k, o in ((2, o2), (3, o3))]
    given.append(up(o1, 1))
    sent = shaped((TOK, HEAD), half)
    h0, *h_sent = call(join_x_kernel, (g0, *g_near), (shaped((TOK, HEAD), full), sent, sent, sent),
                       [((RING, TOK, HEAD), full)])
    g_far = [along_z(h, k) for k, h in enumerate(h_sent, 1)]
    rows = o0 + sum(o.astype(full) for o in given)
    grad_b = h0 + sum(h.astype(full) for h in g_far)
    return narrow(rows), narrow(grad_b)


def solution(mesh):
    inner = Mesh(mesh.devices.reshape(SIZES), AXES)
    tokens = P(AXES, None)

    return jax.shard_map(
        on_device,
        mesh=inner,
        in_specs=(tokens, P(), P(), tokens, tokens),
        out_specs=(tokens, tokens),
        check_vma=False,
    )
```
